32 devices in a mesh: seq: 4 (over z), wt: 8 (over y, x, core).
Axes of the slice: x: 2, y: 2, z: 4, core: 2. Of those that a mesh axis runs over, the one named last changes fastest.
Arguments:
- tokens: bfloat16 [8, 512, 2048], P('wt', 'seq'), may hold values from -6 to 6
- cotangent: bfloat16 [8, 512, 2048], P('wt', 'seq'), may hold values from -6 to 6
- segment_ids: int32 [8, 512], P('wt'), may hold values from 0 to 1, never falling along the last dimension, each value on 1 to 320 neighbouring positions
- expert_routes: int32 [8, 512, 8], P('wt', 'seq'), may hold values from 0 to 15, all different within a row; in each aligned block of 128 rows (0 to 127, 128 to 255, ..., all dimensions but the last counted through in order) at most 128 rows name the same one
- w_qkv: bfloat16 [2048, 6144], P('wt'), may hold values from -0.125 to 0.125
- w_out: bfloat16 [2048, 2048], P('wt'), may hold values from -2 to 2
- w_router: bfloat16 [2048, 16], P('wt'), may hold values from -0.0625 to 0.0625
- w_gate_up: bfloat16 [16, 2048, 2048], P('seq', 'wt'), may hold values from -0.125 to 0.125
- w_down: bfloat16 [16, 1024, 2048], P('seq', 'wt'), may hold values from -0.75 to 0.75
- attn_gain: bfloat16 [2048], P('wt'), may hold values from 0.5 to 1.5
- ffn_gain: bfloat16 [2048], P('wt'), may hold values from 0.5 to 1.5
- q_gain: bfloat16 [128], P('wt'), may hold values from 0.5 to 1.5
- k_gain: bfloat16 [128], P('wt'), may hold values from 0.5 to 1.5
Outputs:
- output: bfloat16 [8, 512, 2048], P('wt', 'seq')
- tokens_grad: float32 [8, 512, 2048], P('wt', 'seq')
- w_qkv_grad: float32 [2048, 6144], P('wt')
- w_out_grad: float32 [2048, 2048], P('wt')
- w_router_grad: float32 [2048, 16], P('wt')
- w_gate_up_grad: float32 [16, 2048, 2048], P('seq', 'wt')
- w_down_grad: float32 [16, 1024, 2048], P('seq', 'wt')
- attn_gain_grad: float32 [2048], P('wt')
- ffn_gain_grad: float32 [2048], P('wt')
- q_gain_grad: float32 [128], P('wt')
- k_gain_grad: float32 [128], P('wt')
The draws below stay inside these ranges and needn't reach their ends.
Inputs may be any that keep to these rules, and one draw needn't show every extreme that they name: `segment_ids`: along a sequence the segment numbers never fall; each of the 2 documents spans 1 to 320 positions. `expert_routes`: A token names 8 different experts; among the 128 tokens of one device no expert is named more than 128 times, a bound that some block reaches.
All inputs are finite; a program needn't handle non-finite values.
Results may differ from the reference program's by a relative error of at most 0.028.
Values may be sent and summed in bfloat16 or wider, within the bound.
A program may use at most 512 MiB of HBM per device.

```python
import math
import jax
import jax.numpy as jnp
import numpy as np
from jax import lax

D = 2048
H = 16
HD = 128
FF = 1024
TOP = 8
TOK_DEV = 128
LENGTH = 512
SEQS = 8
EXPERTS = 16
CAP = 128
SEGS = 2
SEG_MOST = 320
N_SEQ = 4


def steps_of(own_key, extent, cuts, smallest, largest):
    level, own = 1.0, jax.random.fold_in(own_key, 6)
    for dim, shards_of in cuts:
        draws = jnp.exp(jax.random.uniform(jax.random.fold_in(own, dim), (shards_of,), jnp.float32, smallest / len(cuts), largest / len(cuts)))
        level = level * jnp.repeat(draws, extent[dim] // shards_of).reshape([-1 if axis == dim else 1 for axis in range(len(extent))])
    return level


def length_profile(amount, total, limit, lean):
    weights = [(1 << 20) // math.isqrt(standing ** lean) + 1 for standing in range(2, amount + 1)]
    surplus, holding = total - limit - (amount - 1), [1] * (amount - 1)
    while surplus > 0:
        movable = [i for i in range(amount - 1) if holding[i] < limit]
        pool, left = sum([weights[i] for i in movable]), surplus
        for i in movable:
            addition = min(limit - holding[i], max(1, left * weights[i] // pool), surplus)
            holding[i] = holding[i] + addition
            surplus = surplus - addition
    return np.array([limit] + holding)


def ragged(own_key, count, total, reach, skew):
    if count == 2:
        one = jax.random.randint(own_key, (), max(1, total - reach), min(reach, total - 1) + 1)
        return jnp.stack([one, total - one])
    tallies = jnp.asarray(length_profile(count, total, reach, skew), jnp.int32)
    pairs = (count - 1) // 2
    donor, taker = tallies[1:1 + 2 * pairs:2], tallies[2:2 + 2 * pairs:2]
    room = jnp.minimum(donor - 1, reach - taker)
    shifted = jax.random.randint(jax.random.fold_in(own_key, 1), (pairs,), 0, 1 << 20) % (room + 1)
    tallies = tallies.at[1:1 + 2 * pairs:2].set(donor - shifted).at[2:2 + 2 * pairs:2].set(taker + shifted)
    return tallies[jax.random.permutation(jax.random.fold_in(own_key, 2), count)]


def routed_block(own_key, own, number, rows, count, top, bound, lean):
    sequence = jax.random.permutation(own_key, count)
    heavy_load, ordinary = portions_of(count, rows * top, bound, lean, True), portions_of(count, rows * top, bound, lean, False)
    places = jnp.arange(count)

    def named(lengths, rotation):
        used = int((lengths > 0).sum())
        fixed = max(1, used // 4)
        shifted = fixed + (places - fixed + rotation * (used - fixed)) % max(1, count - fixed)
        return jnp.zeros((count,), jnp.int32).at[sequence[jnp.where(places < fixed, places, shifted)]].set(jnp.asarray(lengths, jnp.int32))

    lengths = jnp.where(number % 4 == 0, named(heavy_load, number // 4), named(ordinary, number - number // 4 - 1))
    mixed = jax.random.permutation(jax.random.fold_in(own, 3), count)
    source_of, receiver = mixed[0:count // 2 * 2:2], mixed[1:count // 2 * 2:2]
    margin = jnp.minimum(lengths[source_of] - 1, bound - lengths[receiver]) // 2
    margin = jnp.where((source_of == sequence[0]) | (receiver == sequence[0]) | (lengths[receiver] == 0), 0, jnp.maximum(margin, 0))
    shifted = jax.random.randint(jax.random.fold_in(own, 4), (count // 2,), 0, 1 << 20) % (margin + 1)
    lengths = lengths.at[source_of].add(-shifted).at[receiver].add(shifted)
    labels = jnp.searchsorted(jnp.cumsum(lengths), jnp.arange(rows * top), side="right").astype(jnp.int32)
    table = labels.reshape(top, rows).T
    table = table[jax.random.permutation(jax.random.fold_in(own, 1), rows)]
    rotation = jax.random.randint(jax.random.fold_in(own, 2), (rows, 1), 0, top)
    return jnp.take_along_axis(table, (jnp.arange(top)[None, :] + rotation) % top, axis=1)


def portions_of(amount, total, reach, skew, full):
    weights = [(1 << 20) // math.isqrt(grade ** skew) + 1 for grade in range(1, amount + 1)]
    largest = reach if full else min(reach, max(-(-total // amount), total * weights[0] // sum(weights)))
    least = 1 if total - largest >= amount - 1 else 0
    given, rest = [largest] + [least] * (amount - 1), total - largest - least * (amount - 1)
    while rest > 0:
        candidates = [i for i in range(1, amount) if given[i] < largest] or [i for i in range(1, amount) if given[i] < reach]
        whole, left = sum([weights[i] for i in candidates]), rest
        for i in candidates:
            extra = min(reach - given[i], max(1, left * weights[i] // whole), rest)
            given[i] = given[i] + extra
            rest = rest - extra
    return np.array(given)


def bell_draw(own_key, extent, spread, bound, shards=(), kind=jnp.bfloat16):
    loudness = steps_of(own_key, extent, shards, -0.22, 0.18) if shards else 1.0
    drawn = jax.random.normal(own_key, extent, jnp.float32) * spread * loudness
    return jnp.minimum(jnp.maximum(drawn, -bound), bound).astype(kind)


def setup_inputs(seed: int = 0) -> dict:
    arg_keys = jax.random.split(jax.random.key(seed), 14)
    tokens = bell_draw(arg_keys[0], (SEQS, LENGTH, D), 1.0, 6.0, ((0, 8), (1, 4)))
    cotangent = bell_draw(arg_keys[1], (SEQS, LENGTH, D), 1.0, 6.0, ((0, 8), (1, 4)))
    segment_ids = jax.vmap(lambda own: jnp.searchsorted(jnp.cumsum(ragged(own, SEGS, LENGTH, SEG_MOST, 1)), jnp.arange(LENGTH), side="right"))(jax.random.split(arg_keys[2], SEQS)).reshape((SEQS, LENGTH)).astype(jnp.int32)
    expert_routes_keys = jax.random.split(jax.random.fold_in(arg_keys[3], 1), SEQS * LENGTH // TOK_DEV)
    expert_routes_turns = jax.random.permutation(jax.random.fold_in(arg_keys[3], 3), SEQS * LENGTH // TOK_DEV)
    expert_routes = jax.vmap(lambda own, number: routed_block(jax.random.fold_in(arg_keys[3], 2), own, number, TOK_DEV, EXPERTS, TOP, CAP, 2))(expert_routes_keys, expert_routes_turns).reshape((SEQS, LENGTH, TOP))
    w_qkv = bell_draw(arg_keys[4], (D, 3 * H * HD), D ** -0.5, 0.125, ((0, 8),))
    w_out = bell_draw(arg_keys[5], (H * HD, D), (H * HD // 256) ** -0.5, 2.0, ((0, 8),))
    w_router = bell_draw(arg_keys[6], (D, EXPERTS), (4 * D) ** -0.5, 0.0625, ((0, 8),))
    w_gate_up = bell_draw(arg_keys[7], (EXPERTS, D, 2 * FF), D ** -0.5, 0.125, ((0, 4), (1, 8)))
    w_down = bell_draw(arg_keys[8], (EXPERTS, FF, D), (FF // 16) ** -0.5, 0.75, ((0, 4), (1, 8)))
    attn_gain = jnp.clip(1.0 + 0.1 * jax.random.normal(arg_keys[9], (D,), jnp.float32), 0.5, 1.5).astype(jnp.bfloat16)
    ffn_gain = jnp.clip(1.0 + 0.1 * jax.random.normal(arg_keys[10], (D,), jnp.float32), 0.5, 1.5).astype(jnp.bfloat16)
    q_gain = jnp.clip(1.0 + 0.1 * jax.random.normal(arg_keys[11], (HD,), jnp.float32), 0.5, 1.5).astype(jnp.bfloat16)
    k_gain = jnp.clip(1.0 + 0.1 * jax.random.normal(arg_keys[12], (HD,), jnp.float32), 0.5, 1.5).astype(jnp.bfloat16)
    return {"tokens": tokens, "cotangent": cotangent, "segment_ids": segment_ids, "expert_routes": expert_routes, "w_qkv": w_qkv, "w_out": w_out, "w_router": w_router, "w_gate_up": w_gate_up, "w_down": w_down, "attn_gain": attn_gain, "ffn_gain": ffn_gain, "q_gain": q_gain, "k_gain": k_gain}


EPS = 1e-06
THETA = 50000.0
NEG = -1e+30

@jax.custom_vjp
def low(v):
    return lax.optimization_barrier(v.astype(jnp.bfloat16)).astype(jnp.float32)

@jax.custom_vjp
def low_back(v):
    return v

def low_keep(v):
    return (low(v), None)

def low_pass(kept, grad):
    return (grad,)

def back_keep(v):
    return (v, None)

def back_low(kept, grad):
    return (low(grad),)
low.defvjp(low_keep, low_pass)
low_back.defvjp(back_keep, back_low)

def dense(left, right):
    return jnp.dot(left, right, precision=lax.Precision.HIGHEST, preferred_element_type=jnp.float32)

def normed(values, gain):
    return values * lax.rsqrt(lax.optimization_barrier(jnp.mean(values * values, axis=-1, keepdims=True)) + EPS) * gain

def rotate(values, positions, sign):
    half = values.shape[-1] // 2
    freq = THETA ** (-jnp.arange(half, dtype=jnp.float32) * 2.0 / values.shape[-1])
    angle = positions.astype(jnp.float32)[:, None] * freq[None, :]
    cosine = jnp.cos(angle)[:, None, :]
    sine = sign * jnp.sin(angle)[:, None, :]
    first = values[..., :half]
    second = values[..., half:]
    return jnp.concatenate([first * cosine - second * sine, second * cosine + first * sine], axis=-1)

def sequence_forward(inputs, segments, routes, w_qkv, w_out, w_router, w_gate_up, w_down, attn_gain, ffn_gain, q_gain, k_gain):
    length = inputs.shape[0]
    positions = jnp.arange(length, dtype=jnp.int32)
    hidden = low(normed(inputs, attn_gain))
    projected = low_back(dense(hidden, w_qkv)).reshape(length, 3, H, HD)
    queries = low_back(low(rotate(normed(projected[:, 0], q_gain), positions, 1.0)))
    keys_all = low_back(low(rotate(normed(projected[:, 1], k_gain), positions, 1.0)))
    values_all = low_back(low(projected[:, 2]))
    same_doc = segments[:, None] == segments[None, :]

    def one_head(operands):
        query_one, key_one, value_one = operands
        logits = low_back(dense(query_one, key_one.T) * HD ** (-0.5))
        logits = jnp.where(same_doc, logits, NEG)
        weights = jax.nn.softmax(logits, axis=-1)
        return dense(low(weights), value_one)
    attended = lax.map(jax.checkpoint(one_head), (jnp.swapaxes(queries, 0, 1), jnp.swapaxes(keys_all, 0, 1), jnp.swapaxes(values_all, 0, 1)))
    merged = low_back(low(jnp.swapaxes(attended, 0, 1).reshape(length, H * HD)))
    residual = inputs + low_back(dense(merged, w_out))
    hidden_ffn = low(normed(residual, ffn_gain))
    router_logits = low_back(dense(hidden_ffn, w_router))
    chances = jax.nn.softmax(router_logits, axis=-1)
    picked = jnp.take_along_axis(chances, routes, axis=1)
    gate_values = picked / lax.optimization_barrier(jnp.sum(picked, axis=1, keepdims=True))
    block_rows = length // N_SEQ
    blocks = routes.reshape(N_SEQ, block_rows * TOP)
    onehot_table = (blocks[:, :, None] == jnp.arange(EXPERTS, dtype=jnp.int32)[None, None, :]).astype(jnp.int32)
    ranks = lax.optimization_barrier(jnp.sum((jnp.cumsum(onehot_table, axis=1) - 1) * onehot_table, axis=2)).astype(jnp.int32)
    slots = blocks * CAP + ranks
    block_ids = jnp.broadcast_to(jnp.arange(N_SEQ, dtype=jnp.int32)[:, None], blocks.shape)
    token_ids = block_ids * block_rows + jnp.broadcast_to(jnp.arange(block_rows * TOP, dtype=jnp.int32)[None, :] // TOP, blocks.shape)
    sources = jnp.zeros((N_SEQ, EXPERTS * CAP), jnp.int32).at[block_ids, slots].set(token_ids)
    filled = jnp.zeros((N_SEQ, EXPERTS * CAP), jnp.float32).at[block_ids, slots].set(1.0)
    sources = jnp.transpose(sources.reshape(N_SEQ, EXPERTS, CAP), (1, 0, 2)).reshape(EXPERTS, N_SEQ * CAP)
    filled = jnp.transpose(filled.reshape(N_SEQ, EXPERTS, CAP), (1, 0, 2)).reshape(EXPERTS, N_SEQ * CAP)
    flat_index = (blocks * (N_SEQ * CAP) + block_ids * CAP + ranks).reshape(length, TOP)

    def one_expert(operands):
        index_rows, fill_rows, gate_up_one, down_one = operands
        rows_in = low_back(hidden_ffn[index_rows] * fill_rows[:, None])
        before = low_back(dense(rows_in, gate_up_one))
        activated = low(jax.nn.silu(before[:, :FF]) * before[:, FF:])
        return low_back(low(dense(activated, down_one)))
    expert_out = lax.map(jax.checkpoint(one_expert), (sources, filled, w_gate_up, w_down))
    picked_rows = expert_out.reshape(EXPERTS * N_SEQ * CAP, D)[flat_index]
    return residual + lax.optimization_barrier(jnp.sum(gate_values[:, :, None] * picked_rows, axis=1))

def reference(tokens, cotangent, segment_ids, expert_routes, w_qkv, w_out, w_router, w_gate_up, w_down, attn_gain, ffn_gain, q_gain, k_gain):
    floats = tuple((item.astype(jnp.float32) for item in (tokens, w_qkv, w_out, w_router, w_gate_up, w_down, attn_gain, ffn_gain, q_gain, k_gain)))
    step_fn = jax.checkpoint(sequence_forward)

    def whole(inputs, *weights):

        def step(carry, item):
            return (carry, step_fn(item[0], item[1], item[2], *weights))
        return lax.scan(step, jnp.zeros((), jnp.float32), (inputs, segment_ids, expert_routes))[1]
    result, pull = jax.vjp(whole, *floats)
    grads = pull(cotangent.astype(jnp.float32))
    return (result.astype(jnp.bfloat16), grads[0], grads[1], grads[2], grads[3], grads[4], grads[5], grads[6], grads[7], grads[8], grads[9])
```

```python
import jax
import jax.numpy as jnp
import numpy as np
from jax import lax
from jax.sharding import PartitionSpec as P

H = 16
HD = 128
FF = 1024

EPS = 1e-06
THETA = 50000.0
NEG = -1e30
LANES = 128
BF = jnp.bfloat16
F32 = jnp.float32


def normalize(values):
    factor = lax.rsqrt(jnp.mean(values * values, axis=-1, keepdims=True) + EPS)
    return (values * factor, factor)


def norm_back(grad_normed, normed_values, factor):
    return factor * (
        grad_normed - normed_values * jnp.mean(grad_normed * normed_values, axis=-1, keepdims=True)
    )


def rope_tables(length):
    half = HD // 2
    freq = THETA ** (-jnp.arange(half, dtype=F32) * 2.0 / HD)
    angle = jnp.arange(length, dtype=F32)[:, None] * freq[None, :]
    return jnp.cos(angle)[:, None, :], jnp.sin(angle)[:, None, :]


def rotate(values, cosine, sine):
    half = values.shape[-1] // 2
    first = values[..., :half]
    second = values[..., half:]
    return jnp.concatenate(
        [first * cosine - second * sine, second * cosine + first * sine], axis=-1
    )


def dot(left, right, dims):
    return lax.dot_general(left, right, (dims, ((), ())), preferred_element_type=F32)


def nn(left, right):
    return dot(left, right, ((1,), (0,)))


def nt(left, right):
    return dot(left, right, ((1,), (1,)))


def tn(left, right):
    return dot(left, right, ((0,), (0,)))


def split_two(values):
    high = values.astype(BF)
    low = (values - high.astype(F32)).astype(BF)
    return high, low


def body(
    tokens,
    cotangent,
    segment_ids,
    expert_routes,
    w_qkv,
    w_out,
    w_router,
    w_gate_up,
    w_down,
    attn_gain,
    ffn_gain,
    q_gain,
    k_gain,
):
    seq_total = lax.axis_size("seq")
    wt_total = lax.axis_size("wt")
    seq_me = lax.axis_index("seq")
    rows = tokens.shape[1]
    model = tokens.shape[2]
    length = rows * seq_total
    shard = w_qkv.shape[0]
    local_experts = w_gate_up.shape[0]
    experts = w_router.shape[1]
    heads = H // seq_total
    cols = 3 * heads * HD
    gain_part = q_gain.shape[0]

    tokens_all = lax.all_gather(tokens[0], "seq", axis=0, tiled=True)
    routes_all = lax.all_gather(expert_routes[0], "seq", axis=0, tiled=True)
    w_here = lax.dynamic_slice_in_dim(
        w_qkv.reshape(shard, 3, seq_total, heads * HD), seq_me, 1, axis=2
    ).reshape(shard, cols)
    small = jnp.concatenate(
        [
            w_router,
            attn_gain[:, None],
            ffn_gain[:, None],
            jnp.pad(q_gain, (0, shard - gain_part))[:, None],
            jnp.pad(k_gain, (0, shard - gain_part))[:, None],
        ],
        axis=1,
    )
    small = jnp.pad(small, ((0, 0), (0, LANES - small.shape[1])))
    qkv_full = lax.all_gather(jnp.concatenate([w_here, small], axis=1), "wt", axis=0, tiled=True)
    out_full = lax.all_gather(w_out, "wt", axis=0, tiled=True)
    grad_all = lax.all_gather(cotangent[0], "seq", axis=0, tiled=True)
    expert_full = [
        lax.all_gather(jnp.concatenate([w_gate_up[e], w_down[e]], axis=0), "wt", axis=0)
        for e in range(local_experts)
    ]

    small_full = qkv_full[:, cols:]
    router_full = small_full[:, :experts]
    picker = np.zeros((8, LANES), np.float32)
    for row in range(4):
        picker[row, experts + row] = 1.0
    gain_rows = nt(jnp.asarray(picker, BF), small_full)
    gain_attn = gain_rows[0]
    gain_ffn = gain_rows[1]
    gain_query = gain_rows[2].reshape(wt_total, shard)[:, :gain_part].reshape(HD)
    gain_key = gain_rows[3].reshape(wt_total, shard)[:, :gain_part].reshape(HD)

    segments = segment_ids[0]
    same = segments[:, None] == segments[None, :]
    cosine, sine = rope_tables(length)
    normed_all, _ = normalize(tokens_all.astype(F32))
    hidden = (normed_all * gain_attn).astype(BF)
    projected = nn(hidden, qkv_full)[:, :cols].reshape(length, 3, heads, HD)
    normed_q, factor_q = normalize(projected[:, 0])
    normed_k, factor_k = normalize(projected[:, 1])
    queries = jnp.swapaxes(rotate(normed_q * gain_query, cosine, sine).astype(BF), 0, 1)
    keys = jnp.swapaxes(rotate(normed_k * gain_key, cosine, sine).astype(BF), 0, 1)
    values = jnp.swapaxes(projected[:, 2].astype(BF), 0, 1)
    scale = HD ** (-0.5)

    def bmm(left, right, dims):
        return lax.dot_general(left, right, (dims, ((0,), (0,))), preferred_element_type=F32)

    logits = jnp.where(same[None], bmm(queries, keys, ((2,), (2,))) * scale, NEG)
    powers = jnp.exp(logits - jnp.max(logits, axis=-1, keepdims=True))
    weights = powers / jnp.sum(powers, axis=-1, keepdims=True)
    weights_low = weights.astype(BF)
    attended = bmm(weights_low, values, ((2,), (1,))).astype(BF)
    merged = lax.all_to_all(
        jnp.swapaxes(attended, 0, 1), "seq", split_axis=0, concat_axis=1, tiled=True
    ).reshape(rows, H * HD)

    inputs = tokens[0].astype(F32)
    residual = inputs + nn(merged, out_full)
    normed_f, factor_f = normalize(residual)
    hidden_own = (normed_f * gain_ffn).astype(BF)
    hidden_ffn = lax.all_gather(hidden_own, "seq", axis=0, tiled=True)

    chances = jax.nn.softmax(nn(hidden_ffn, router_full), axis=-1)
    expert_ids = jnp.arange(experts, dtype=jnp.int32)
    routed = jnp.any(routes_all[:, :, None] == expert_ids[None, None, :], axis=1)
    picked = jnp.where(routed, chances, 0.0)
    picked_total = jnp.sum(picked, axis=1, keepdims=True)
    gates = picked / picked_total
    gates_here = lax.dynamic_slice_in_dim(gates, seq_me * local_experts, local_experts, axis=1)

    out_part = jnp.zeros((length, model), F32)
    grad_hidden_part = jnp.zeros((length, model), F32)
    gate_grads = []
    expert_grads = []
    for e in range(local_experts):
        gate = gates_here[:, e : e + 1]
        gate_up = expert_full[e][:, : model // wt_total].reshape(model, 2 * FF)
        down = expert_full[e][:, model // wt_total :].reshape(FF, model)
        before = nn(hidden_ffn, gate_up)
        gate_part = before[:, :FF]
        up_part = before[:, FF:]
        sigmoid_gate = jax.nn.sigmoid(gate_part)
        silu_gate = gate_part * sigmoid_gate
        activated = silu_gate * up_part
        scaled = (gate * activated).astype(BF)
        grad_act = nt(grad_all, down)
        gate_grads.append(jnp.sum(grad_act * activated, axis=1, keepdims=True))
        grad_act = grad_act * gate
        grad_gate = grad_act * up_part * sigmoid_gate * (1.0 + gate_part * (1.0 - sigmoid_gate))
        grad_up = grad_act * silu_gate
        grad_before = jnp.concatenate([grad_gate, grad_up], axis=-1).astype(BF)
        out_part = out_part + nn(scaled, down)
        grad_hidden_part = grad_hidden_part + nt(grad_before, gate_up)
        gate_up_grad = tn(hidden_ffn, grad_before).astype(BF)
        down_grad = tn(scaled, grad_all).astype(BF)
        joined = jnp.concatenate(
            [
                gate_up_grad.reshape(wt_total, model // wt_total, 2 * FF),
                down_grad.reshape(wt_total, FF // wt_total, model),
            ],
            axis=1,
        )
        expert_grads.append(
            lax.psum_scatter(joined, "wt", scatter_dimension=0, tiled=False).astype(F32)
        )
    gate_up_out = jnp.stack([g[: model // wt_total] for g in expert_grads])
    down_out = jnp.stack([g[model // wt_total :] for g in expert_grads])

    gate_grad_part = jnp.concatenate(gate_grads, axis=1)
    gate_high, gate_low = split_two(gate_grad_part)

    def spread(part):
        wide = jnp.zeros((length, experts), BF)
        return lax.dynamic_update_slice(wide, part, (0, seq_me * local_experts))

    returned = lax.psum_scatter(
        jnp.concatenate(
            [grad_hidden_part.astype(BF), spread(gate_high), spread(gate_low)], axis=1
        ),
        "seq",
        scatter_dimension=0,
        tiled=True,
    ).astype(F32)
    grad_hidden = returned[:, :model]
    gate_grad = returned[:, model : model + experts] + returned[:, model + experts :]
    moe_out = lax.psum_scatter(
        out_part.astype(BF), "seq", scatter_dimension=0, tiled=True
    ).astype(F32)
    output = (residual + moe_out).astype(BF)

    def own(full):
        return lax.dynamic_slice_in_dim(full, seq_me * rows, rows, axis=0)

    chances_own = own(chances)
    routed_own = own(routed)
    gates_own = own(gates)
    inner_gate = jnp.sum(gate_grad * gates_own, axis=1, keepdims=True)
    grad_chances = jnp.where(routed_own, (gate_grad - inner_gate) / own(picked_total), 0.0)
    grad_logits = (
        chances_own
        * (grad_chances - jnp.sum(grad_chances * chances_own, axis=1, keepdims=True))
    ).astype(BF)
    grad_hidden = grad_hidden + nt(grad_logits, router_full)
    router_grad = tn(hidden_own, grad_logits)
    ffn_gain_grad = jnp.sum(grad_hidden * normed_f, axis=0)
    grad_residual = cotangent[0].astype(F32) + norm_back(
        grad_hidden * gain_ffn, normed_f, factor_f
    )
    grad_branch = grad_residual.astype(BF)
    grad_merged = nt(grad_branch, out_full).astype(BF).reshape(rows, H, HD)
    grad_heads = jnp.swapaxes(
        lax.all_to_all(grad_merged, "seq", split_axis=1, concat_axis=0, tiled=True), 0, 1
    )
    out_grad = lax.psum_scatter(
        tn(merged, grad_branch).astype(BF), "wt", scatter_dimension=0, tiled=True
    )
    out_grad = lax.psum(out_grad, "seq").astype(F32)

    grad_weights = bmm(grad_heads, values, ((2,), (2,)))
    inner = jnp.sum(weights * grad_weights, axis=-1, keepdims=True)
    grad_scores = (weights * (grad_weights - inner)).astype(BF)
    grad_q = jnp.swapaxes(bmm(grad_scores, keys, ((2,), (1,))), 0, 1) * scale
    grad_k = jnp.swapaxes(bmm(grad_scores, queries, ((1,), (1,))), 0, 1) * scale
    grad_v = jnp.swapaxes(bmm(weights_low, grad_heads, ((1,), (1,))), 0, 1)
    grad_q_normed = rotate(grad_q, cosine, -sine)
    grad_k_normed = rotate(grad_k, cosine, -sine)
    q_gain_grad = jnp.sum(grad_q_normed * normed_q, axis=(0, 1))
    k_gain_grad = jnp.sum(grad_k_normed * normed_k, axis=(0, 1))
    grad_q_raw = norm_back(grad_q_normed * gain_query, normed_q, factor_q)
    grad_k_raw = norm_back(grad_k_normed * gain_key, normed_k, factor_k)
    grad_projected = (
        jnp.stack([grad_q_raw, grad_k_raw, grad_v], axis=1).reshape(length, cols).astype(BF)
    )
    qkv_grad = tn(hidden, grad_projected)
    grad_normed_part = nt(
        jnp.pad(grad_projected, ((0, 0), (0, LANES))), qkv_full
    )
    attn_gain_grad = jnp.sum(grad_normed_part * normed_all, axis=0)
    grad_normed_own = lax.psum_scatter(
        grad_normed_part.astype(BF), "seq", scatter_dimension=0, tiled=True
    ).astype(F32)
    normed_a, factor_a = normalize(inputs)
    tokens_grad = grad_residual + norm_back(grad_normed_own * gain_attn, normed_a, factor_a)

    def gain_column(vector):
        return jnp.pad(
            vector.reshape(wt_total, gain_part), ((0, 0), (0, shard - gain_part))
        ).reshape(model, 1)

    small_grad = jnp.concatenate(
        [
            router_grad,
            attn_gain_grad[:, None],
            ffn_gain_grad[:, None],
            gain_column(q_gain_grad),
            gain_column(k_gain_grad),
        ],
        axis=1,
    )
    small_grad = jnp.pad(small_grad, ((0, 0), (0, LANES - small_grad.shape[1])))
    scattered = lax.psum_scatter(
        jnp.concatenate([qkv_grad, small_grad], axis=1).astype(BF),
        "wt",
        scatter_dimension=0,
        tiled=True,
    )
    collected = lax.all_gather(scattered, "seq", axis=0).astype(F32)
    qkv_out = (
        collected[:, :, :cols]
        .reshape(seq_total, shard, 3, heads * HD)
        .transpose(1, 2, 0, 3)
        .reshape(shard, 3 * H * HD)
    )
    small_out = jnp.sum(collected[:, :, cols:], axis=0)
    return (
        output[None],
        tokens_grad[None],
        qkv_out,
        out_grad,
        small_out[:, :experts],
        gate_up_out,
        down_out,
        small_out[:, experts],
        small_out[:, experts + 1],
        small_out[:gain_part, experts + 2],
        small_out[:gain_part, experts + 3],
    )


def solution(mesh):
    in_specs = (
        P("wt", "seq", None),
        P("wt", "seq", None),
        P("wt", None),
        P("wt", "seq", None),
        P("wt", None),
        P("wt", None),
        P("wt", None),
        P("seq", "wt", None),
        P("seq", "wt", None),
        P("wt"),
        P("wt"),
        P("wt"),
        P("wt"),
    )
    out_specs = (
        P("wt", "seq", None),
        P("wt", "seq", None),
        P("wt", None),
        P("wt", None),
        P("wt", None),
        P("seq", "wt", None),
        P("seq", "wt", None),
        P("wt"),
        P("wt"),
        P("wt"),
        P("wt"),
    )
    return jax.shard_map(body, mesh=mesh, in_specs=in_specs, out_specs=out_specs, check_vma=False)
```

```python
import jax
import jax.numpy as jnp
import numpy as np
from jax import lax
from jax.sharding import PartitionSpec as P

H = 16
HD = 128
FF = 1024

EPS = 1e-06
THETA = 50000.0
NEG = -1e30
LANES = 128
BF = jnp.bfloat16
F32 = jnp.float32


def normalize(values):
    factor = lax.rsqrt(jnp.mean(values * values, axis=-1, keepdims=True) + EPS)
    return (values * factor, factor)


def norm_back(grad_normed, normed_values, factor):
    return factor * (
        grad_normed - normed_values * jnp.mean(grad_normed * normed_values, axis=-1, keepdims=True)
    )


def rope_tables(length):
    half = HD // 2
    freq = THETA ** (-jnp.arange(half, dtype=F32) * 2.0 / HD)
    angle = jnp.arange(length, dtype=F32)[:, None] * freq[None, :]
    return jnp.cos(angle)[:, None, :], jnp.sin(angle)[:, None, :]


def rotate(values, cosine, sine):
    half = values.shape[-1] // 2
    first = values[..., :half]
    second = values[..., half:]
    return jnp.concatenate(
        [first * cosine - second * sine, second * cosine + first * sine], axis=-1
    )


def dot(left, right, dims):
    return lax.dot_general(left, right, (dims, ((), ())), preferred_element_type=F32)


def nn(left, right):
    return dot(left, right, ((1,), (0,)))


def nt(left, right):
    return dot(left, right, ((1,), (1,)))


def tn(left, right):
    return dot(left, right, ((0,), (0,)))


def split_two(values):
    high = values.astype(BF)
    low = (values - high.astype(F32)).astype(BF)
    return high, low


def swap(values, bit):
    total = lax.axis_size("wt")
    return lax.ppermute(values, "wt", [(i, i ^ bit) for i in range(total)])


def bits_of(chips, route):
    bits = []
    while 1 << len(bits) < chips:
        bits.append(1 << len(bits))
    return bits[::-1] if route else bits


def gather_chips(own, route, chips):
    bits = bits_of(chips, route)
    pieces = {0: own}
    for place, bit in enumerate(bits):
        for mask in list(pieces):
            pieces[mask ^ bit] = swap(pieces[mask], 2 * bit)
    return [pieces[mask] for mask in range(chips)]


def scatter_chips(parts, route, chips):
    bits = bits_of(chips, route)
    held = dict(enumerate(parts))
    for place, bit in enumerate(bits):
        for mask in [m for m in held if m & bit]:
            arrived = swap(held.pop(mask), 2 * bit)
            total = held[mask ^ bit].astype(F32) + arrived.astype(F32)
            rest = [b for b in bits[place + 1 :] if (mask ^ bit) & b]
            held[mask ^ bit] = total.astype(BF) if rest else total
    return held[0]


def body(
    tokens,
    cotangent,
    segment_ids,
    expert_routes,
    w_qkv,
    w_out,
    w_router,
    w_gate_up,
    w_down,
    attn_gain,
    ffn_gain,
    q_gain,
    k_gain,
):
    seq_total = lax.axis_size("seq")
    wt_total = lax.axis_size("wt")
    seq_me = lax.axis_index("seq")
    wt_me = lax.axis_index("wt")
    core = wt_me % 2
    chip = wt_me // 2
    chips = wt_total // 2
    first_core = core == 0
    rows = tokens.shape[1]
    model = tokens.shape[2]
    length = rows * seq_total
    shard = model // wt_total
    local_experts = w_gate_up.shape[0]
    experts = w_router.shape[1]
    heads = H // seq_total
    part = heads * HD
    cols = 3 * part
    gain_part = q_gain.shape[0]
    half = model // 2
    order = [2 * m for m in range(chips)] + [2 * m + 1 for m in range(chips)]
    slim = FF // wt_total

    def pick_blocks(values, places, width):
        return jnp.concatenate(
            [lax.dynamic_slice_in_dim(values, place * width, width, axis=1) for place in places],
            axis=1,
        )

    def to_relative(values):
        return pick_blocks(values, [wt_me ^ mask for mask in order], shard)

    def from_relative(values):
        masks = [wt_me ^ device for device in range(wt_total)]
        return pick_blocks(values, [mask // 2 + (mask % 2) * chips for mask in masks], shard)

    def by_chip(values):
        return pick_blocks(values, [chip ^ mask for mask in range(chips)], 2 * shard)

    small = jnp.concatenate(
        [
            w_router,
            attn_gain[:, None],
            ffn_gain[:, None],
            jnp.pad(q_gain, (0, shard - gain_part))[:, None],
            jnp.pad(k_gain, (0, shard - gain_part))[:, None],
        ],
        axis=1,
    )
    small = jnp.pad(small, ((0, 0), (0, LANES - small.shape[1])))
    qkv_here = jnp.concatenate(
        [
            lax.dynamic_slice_in_dim(w_qkv, kind * H * HD + seq_me * part, part, axis=1)
            for kind in range(3)
        ]
        + [small],
        axis=1,
    )
    token_ids = jnp.arange(experts, dtype=jnp.int32)
    routed_own = jnp.any(expert_routes[0][:, :, None] == token_ids[None, None, :], axis=1)
    tokens_sent = jnp.concatenate(
        [
            to_relative(tokens[0]),
            jnp.pad(routed_own.astype(BF), ((0, 0), (0, LANES - experts))),
        ],
        axis=1,
    )
    tokens_got = lax.all_gather(tokens_sent, "seq", axis=0, tiled=True)
    tokens_all = tokens_got[:, :model]
    routed = tokens_got[:, model : model + experts] > 0.5

    qkv_pieces = gather_chips(qkv_here, 0, chips)
    out_pieces = gather_chips(w_out, 1, chips)
    qkv_even = jnp.concatenate(qkv_pieces, axis=0)
    qkv_odd = swap(qkv_even, 1)
    out_even = jnp.concatenate(out_pieces, axis=0)
    out_odd = swap(out_even, 1)

    def columns_of(values, which):
        return jnp.concatenate(
            [
                values[:, (2 * j + which) * slim : (2 * j + which + 1) * slim]
                for j in range(wt_total)
            ],
            axis=1,
        )

    gate_ups = []
    downs = []
    tie = qkv_pieces[-1]
    ties = [qkv_pieces[-1], out_pieces[-1]]
    for e in range(local_experts):
        low_half = columns_of(w_gate_up[e], 0)
        high_half = columns_of(w_gate_up[e], 1)
        mine = jnp.where(first_core, low_half, high_half)
        others = swap(jnp.where(first_core, high_half, low_half), 1)
        pair = jnp.where(
            first_core,
            jnp.concatenate([mine, others], axis=0),
            jnp.concatenate([others, mine], axis=0),
        )
        down_own = w_down[e]
        pair, down_own, _ = lax.optimization_barrier((pair, down_own, tuple(ties)))
        pieces = gather_chips(pair, e % 2, chips)
        down_pieces = gather_chips(down_own, 1 - e % 2, chips)
        ties = [pieces[-1], down_pieces[-1]]
        gate_ups.append(jnp.concatenate(pieces, axis=0))
        down = jnp.zeros((FF // 2, model), BF)
        for mask in range(chips):
            down = lax.dynamic_update_slice_in_dim(
                down, down_pieces[mask], (chip ^ mask) * slim, axis=0
            )
        downs.append(down)

    grad_seq = lax.all_gather(cotangent[0], "seq", axis=0, tiled=True)
    grad_two = jnp.concatenate([grad_seq, swap(grad_seq, 1)], axis=0)

    small_relative = jnp.concatenate([qkv_even[:, cols:], qkv_odd[:, cols:]], axis=0)
    router = jnp.concatenate(
        [
            lax.dynamic_slice_in_dim(
                small_relative, (mask + (side ^ core) * chips) * shard, shard, axis=0
            )
            for mask in range(chips)
            for side in range(2)
        ],
        axis=0,
    )[:, :experts]
    picker = np.zeros((8, LANES), np.float32)
    for row in range(4):
        picker[row, experts + row] = 1.0
    gain_rows = nt(jnp.asarray(picker, BF), small_relative)
    gain_attn_relative = gain_rows[0]
    gain_rows = from_relative(gain_rows)
    gain_attn = gain_rows[0]
    gain_ffn = gain_rows[1]
    gain_query = gain_rows[2].reshape(wt_total, shard)[:, :gain_part].reshape(HD)
    gain_key = gain_rows[3].reshape(wt_total, shard)[:, :gain_part].reshape(HD)

    segments = segment_ids[0]
    same = segments[:, None] == segments[None, :]
    cosine, sine = rope_tables(length)
    normed_all, _ = normalize(tokens_all.astype(F32))
    hidden = (normed_all * gain_attn_relative).astype(BF)
    projected = nn(hidden[:, :half], qkv_even[:, :cols]) + nn(hidden[:, half:], qkv_odd[:, :cols])
    projected = projected.reshape(length, 3, heads, HD)
    normed_q, factor_q = normalize(projected[:, 0])
    normed_k, factor_k = normalize(projected[:, 1])
    queries = jnp.swapaxes(rotate(normed_q * gain_query, cosine, sine).astype(BF), 0, 1)
    keys = jnp.swapaxes(rotate(normed_k * gain_key, cosine, sine).astype(BF), 0, 1)
    values = jnp.swapaxes(projected[:, 2].astype(BF), 0, 1)
    scale = HD ** (-0.5)

    def bmm(left, right, dims):
        return lax.dot_general(left, right, (dims, ((0,), (0,))), preferred_element_type=F32)

    logits = jnp.where(same[None], bmm(queries, keys, ((2,), (2,))) * scale, NEG)
    powers = jnp.exp(logits - jnp.max(logits, axis=-1, keepdims=True))
    weights = powers / jnp.sum(powers, axis=-1, keepdims=True)
    weights_low = weights.astype(BF)
    attended = bmm(weights_low, values, ((2,), (1,))).astype(BF)
    merged = lax.all_to_all(
        jnp.swapaxes(attended, 0, 1), "seq", split_axis=0, concat_axis=1, tiled=True
    ).reshape(rows, H * HD)
    merged = to_relative(merged)

    inputs = tokens[0].astype(F32)
    residual = inputs + nn(merged[:, :half], out_even) + nn(merged[:, half:], out_odd)
    normed_f, factor_f = normalize(residual)
    hidden_own = (normed_f * gain_ffn).astype(BF)
    hidden_seq = lax.all_gather(by_chip(hidden_own), "seq", axis=0, tiled=True)
    hidden_two = jnp.concatenate([hidden_seq, swap(hidden_seq, 1)], axis=0)

    chances = jax.nn.softmax(nn(hidden_seq, router), axis=-1)
    picked = jnp.where(routed, chances, 0.0)
    picked_total = jnp.sum(picked, axis=1, keepdims=True)
    gates = picked / picked_total
    gates_seq = lax.dynamic_slice_in_dim(gates, seq_me * local_experts, local_experts, axis=1)
    gates_two = jnp.concatenate([gates_seq, swap(gates_seq, 1)], axis=0)

    out_part = jnp.zeros((2 * length, model), F32)
    grad_hidden_part = jnp.zeros((2 * length, model), F32)
    gate_grads = []
    wide_grads = []
    scaled_all = []
    for e in range(local_experts):
        gate = gates_two[:, e : e + 1]
        before = nn(hidden_two, gate_ups[e])
        gate_part = before[:, : FF // 2]
        up_part = before[:, FF // 2 :]
        sigmoid_gate = jax.nn.sigmoid(gate_part)
        silu_gate = gate_part * sigmoid_gate
        activated = silu_gate * up_part
        scaled = (gate * activated).astype(BF)
        grad_act = nt(grad_two, downs[e])
        gate_grads.append(jnp.sum(grad_act * activated, axis=1, keepdims=True))
        grad_act = grad_act * gate
        grad_gate = grad_act * up_part * sigmoid_gate * (1.0 + gate_part * (1.0 - sigmoid_gate))
        grad_up = grad_act * silu_gate
        grad_before = jnp.concatenate([grad_gate, grad_up], axis=-1).astype(BF)
        out_part = out_part + nn(scaled, downs[e])
        grad_hidden_part = grad_hidden_part + nt(grad_before, gate_ups[e])
        wide_grads.append(grad_before)
        scaled_all.append(scaled)

    gate_grad_two = jnp.concatenate(gate_grads, axis=1)
    gate_grad_part = gate_grad_two[:length] + swap(gate_grad_two[length:], 1)
    gate_high, gate_low = split_two(gate_grad_part)
    grad_hidden_low = (
        grad_hidden_part[:length] + swap(grad_hidden_part[length:].astype(BF), 1).astype(F32)
    ).astype(BF)

    def spread(values):
        wide = jnp.zeros((length, experts), BF)
        return lax.dynamic_update_slice(wide, values, (0, seq_me * local_experts))

    returned = lax.psum_scatter(
        jnp.concatenate([grad_hidden_low, spread(gate_high), spread(gate_low)], axis=1),
        "seq",
        scatter_dimension=0,
        tiled=True,
    ).astype(F32)
    gate_grad = returned[:, model : model + experts] + returned[:, model + experts :]
    out_low = (out_part[:length] + swap(out_part[length:].astype(BF), 1).astype(F32)).astype(BF)
    out_low, returned = lax.optimization_barrier((out_low, returned))
    moe_out = lax.psum_scatter(out_low, "seq", scatter_dimension=0, tiled=True).astype(F32)
    output = (residual + moe_out).astype(BF)

    gate_up_rows = []
    down_rows = []
    for e in range(local_experts):
        parts = [
            tn(hidden_two[:, mask * 2 * shard : (mask + 1) * 2 * shard], wide_grads[e]).astype(BF)
            for mask in range(chips)
        ]
        down_grad = tn(scaled_all[e], grad_two).astype(BF)
        down_parts = [
            lax.dynamic_slice_in_dim(down_grad, (chip ^ mask) * slim, slim, axis=0)
            for mask in range(chips)
        ]
        summed = scatter_chips(parts, e % 2, chips).astype(BF)
        down_rows.append(scatter_chips(down_parts, 1 - e % 2, chips))
        kept = lax.dynamic_slice_in_dim(summed, core * shard, shard, axis=0)
        sent = lax.dynamic_slice_in_dim(summed, (1 - core) * shard, shard, axis=0)
        got = swap(sent, 1)
        low_half = jnp.where(first_core, kept, got)
        high_half = jnp.where(first_core, got, kept)
        gate_up_rows.append(
            jnp.concatenate(
                [
                    source[:, j * slim : (j + 1) * slim]
                    for j in range(wt_total)
                    for source in (low_half, high_half)
                ],
                axis=1,
            ).astype(F32)
        )
    gate_up_out = jnp.stack(gate_up_rows)
    down_out = jnp.stack(down_rows)

    def own(full):
        return lax.dynamic_slice_in_dim(full, seq_me * rows, rows, axis=0)

    chances_own = own(chances)
    gates_own = own(gates)
    inner_gate = jnp.sum(gate_grad * gates_own, axis=1, keepdims=True)
    grad_chances = jnp.where(routed_own, (gate_grad - inner_gate) / own(picked_total), 0.0)
    grad_logits = (
        chances_own
        * (grad_chances - jnp.sum(grad_chances * chances_own, axis=1, keepdims=True))
    ).astype(BF)
    grad_hidden = by_chip(returned[:, :model] + nt(grad_logits, router))
    router_grad = tn(
        to_relative(hidden_own), jnp.pad(grad_logits, ((0, 0), (0, LANES - experts)))
    )
    ffn_gain_grad = jnp.sum(grad_hidden * normed_f, axis=0)
    grad_residual = cotangent[0].astype(F32) + norm_back(
        grad_hidden * gain_ffn, normed_f, factor_f
    )
    grad_branch = grad_residual.astype(BF)
    grad_merged = jnp.concatenate([nt(grad_branch, out_even), nt(grad_branch, out_odd)], axis=1)
    grad_merged = from_relative(grad_merged.astype(BF)).reshape(rows, H, HD)
    grad_heads = jnp.swapaxes(
        lax.all_to_all(grad_merged, "seq", split_axis=1, concat_axis=0, tiled=True), 0, 1
    )

    def scatter_rows(left, right, route):
        sent = tn(left[:, half:], right).astype(BF)
        kept = (tn(left[:, :half], right) + swap(sent, 1).astype(F32)).astype(BF)
        parts = [kept[mask * shard : (mask + 1) * shard] for mask in range(chips)]
        return scatter_chips(parts, route, chips).astype(BF)

    out_grad = lax.psum(scatter_rows(merged, grad_branch, 1), "seq").astype(F32)

    grad_v = jnp.swapaxes(bmm(weights_low, grad_heads, ((1,), (1,))), 0, 1)
    grad_weights = bmm(grad_heads, values, ((2,), (2,)))
    inner = jnp.sum(weights * grad_weights, axis=-1, keepdims=True)
    grad_scores = (weights * (grad_weights - inner)).astype(BF)
    grad_q = jnp.swapaxes(bmm(grad_scores, keys, ((2,), (1,))), 0, 1) * scale
    grad_k = jnp.swapaxes(bmm(grad_scores, queries, ((1,), (1,))), 0, 1) * scale
    grad_q_normed = rotate(grad_q, cosine, -sine)
    grad_k_normed = rotate(grad_k, cosine, -sine)
    q_gain_grad = jnp.sum(grad_q_normed * normed_q, axis=(0, 1))
    k_gain_grad = jnp.sum(grad_k_normed * normed_k, axis=(0, 1))
    grad_q_raw = norm_back(grad_q_normed * gain_query, normed_q, factor_q)
    grad_k_raw = norm_back(grad_k_normed * gain_key, normed_k, factor_k)
    grads = [g.reshape(length, part).astype(BF) for g in (grad_q_raw, grad_k_raw, grad_v)]
    grad_projected = jnp.concatenate(grads, axis=1)
    grad_normed_part = jnp.concatenate(
        [nt(grad_projected, qkv_even[:, :cols]), nt(grad_projected, qkv_odd[:, :cols])], axis=1
    )
    attn_gain_grad = jnp.sum(grad_normed_part * normed_all, axis=0)
    grad_normed_own = lax.psum_scatter(
        grad_normed_part.astype(BF), "seq", scatter_dimension=0, tiled=True
    ).astype(F32)
    grad_normed_own = from_relative(grad_normed_own)
    normed_a, factor_a = normalize(inputs)
    tokens_grad = grad_residual + norm_back(grad_normed_own * gain_attn, normed_a, factor_a)

    def gain_line(vector):
        return jnp.pad(
            vector.reshape(wt_total, gain_part), ((0, 0), (0, shard - gain_part))
        ).reshape(model)

    lines = to_relative(
        jnp.stack([ffn_gain_grad, gain_line(q_gain_grad), gain_line(k_gain_grad)])
    )
    lines = jnp.concatenate([attn_gain_grad[None], lines, jnp.zeros((4, model), F32)], axis=0)
    small_grad = router_grad + tn(lines.astype(BF), jnp.asarray(picker, BF))
    small_sent = small_grad[half:].astype(BF)
    small_kept = (small_grad[:half] + swap(small_sent, 1).astype(F32)).astype(BF)
    small_sum = scatter_chips(
        [small_kept[mask * shard : (mask + 1) * shard] for mask in range(chips)], 1, chips
    ).astype(BF)
    value_sum = scatter_rows(hidden, grads[2], 0)
    query_sum = scatter_rows(hidden, grads[0], 1)
    key_sum = scatter_rows(hidden, grads[1], 0)
    collected_value = lax.all_gather(value_sum, "seq", axis=0)
    collected = lax.all_gather(
        jnp.concatenate([query_sum, key_sum, small_sum], axis=1), "seq", axis=0
    )
    qkv_out = jnp.concatenate(
        [collected[z, :, :part] for z in range(seq_total)]
        + [collected[z, :, part : 2 * part] for z in range(seq_total)]
        + [collected_value[z] for z in range(seq_total)],
        axis=1,
    ).astype(F32)
    small_out = jnp.sum(collected[:, :, 2 * part :].astype(F32), axis=0)
    return (
        output[None],
        tokens_grad[None],
        qkv_out,
        out_grad,
        small_out[:, :experts],
        gate_up_out,
        down_out,
        small_out[:, experts],
        small_out[:, experts + 1],
        small_out[:gain_part, experts + 2],
        small_out[:gain_part, experts + 3],
    )


def solution(mesh):
    in_specs = (
        P("wt", "seq", None),
        P("wt", "seq", None),
        P("wt", None),
        P("wt", "seq", None),
        P("wt", None),
        P("wt", None),
        P("wt", None),
        P("seq", "wt", None),
        P("seq", "wt", None),
        P("wt"),
        P("wt"),
        P("wt"),
        P("wt"),
    )
    out_specs = (
        P("wt", "seq", None),
        P("wt", "seq", None),
        P("wt", None),
        P("wt", None),
        P("wt", None),
        P("seq", "wt", None),
        P("seq", "wt", None),
        P("wt"),
        P("wt"),
        P("wt"),
        P("wt"),
    )
    return jax.shard_map(body, mesh=mesh, in_specs=in_specs, out_specs=out_specs, check_vma=False)
```

```python
import jax
import jax.numpy as jnp
import numpy as np
from jax import lax
from jax.sharding import PartitionSpec as P

H = 16
HD = 128
FF = 1024

EPS = 1e-06
THETA = 50000.0
NEG = -1e30
LANES = 128
BF = jnp.bfloat16
F32 = jnp.float32


def normalize(values):
    factor = lax.rsqrt(jnp.mean(values * values, axis=-1, keepdims=True) + EPS)
    return (values * factor, factor)


def norm_back(grad_normed, normed_values, factor):
    return factor * (
        grad_normed - normed_values * jnp.mean(grad_normed * normed_values, axis=-1, keepdims=True)
    )


def rope_tables(length):
    half = HD // 2
    freq = THETA ** (-jnp.arange(half, dtype=F32) * 2.0 / HD)
    angle = jnp.arange(length, dtype=F32)[:, None] * freq[None, :]
    return jnp.cos(angle)[:, None, :], jnp.sin(angle)[:, None, :]


def rotate(values, cosine, sine):
    half = values.shape[-1] // 2
    first = values[..., :half]
    second = values[..., half:]
    return jnp.concatenate(
        [first * cosine - second * sine, second * cosine + first * sine], axis=-1
    )


def dot(left, right, dims):
    return lax.dot_general(left, right, (dims, ((), ())), preferred_element_type=F32)


def nn(left, right):
    return dot(left, right, ((1,), (0,)))


def nt(left, right):
    return dot(left, right, ((1,), (1,)))


def tn(left, right):
    return dot(left, right, ((0,), (0,)))


def split_two(values):
    high = values.astype(BF)
    low = (values - high.astype(F32)).astype(BF)
    return high, low


def swap(values, bit):
    total = lax.axis_size("wt")
    return lax.ppermute(values, "wt", [(i, i ^ bit) for i in range(total)])


def bits_of(chips, route):
    bits = []
    while 1 << len(bits) < chips:
        bits.append(1 << len(bits))
    return bits[::-1] if route else bits


def gather_chips(own, route, chips):
    bits = bits_of(chips, route)
    pieces = {0: own}
    for place, bit in enumerate(bits):
        for mask in list(pieces):
            pieces[mask ^ bit] = swap(pieces[mask], 2 * bit)
    return [pieces[mask] for mask in range(chips)]


def send_first(parts, route, chips):
    bit = bits_of(chips, route)[0]
    return {mask: swap(parts[mask], 2 * bit) for mask in range(chips) if mask & bit}


def scatter_chips(parts, route, chips, first=None):
    bits = bits_of(chips, route)
    held = dict(enumerate(parts))
    if first is None:
        first = send_first(parts, route, chips)
    for place, bit in enumerate(bits):
        for mask in [m for m in held if m & bit]:
            sent = held.pop(mask)
            arrived = swap(sent, 2 * bit) if place else first[mask]
            total = held[mask ^ bit].astype(F32) + arrived.astype(F32)
            rest = [b for b in bits[place + 1 :] if (mask ^ bit) & b]
            held[mask ^ bit] = total.astype(BF) if rest else total
    return held[0]


def body(
    tokens,
    cotangent,
    segment_ids,
    expert_routes,
    w_qkv,
    w_out,
    w_router,
    w_gate_up,
    w_down,
    attn_gain,
    ffn_gain,
    q_gain,
    k_gain,
):
    seq_total = lax.axis_size("seq")
    wt_total = lax.axis_size("wt")
    seq_me = lax.axis_index("seq")
    wt_me = lax.axis_index("wt")
    core = wt_me % 2
    chip = wt_me // 2
    chips = wt_total // 2
    first_core = core == 0
    rows = tokens.shape[1]
    model = tokens.shape[2]
    length = rows * seq_total
    shard = model // wt_total
    local_experts = w_gate_up.shape[0]
    experts = w_router.shape[1]
    heads = H // seq_total
    part = heads * HD
    cols = 3 * part
    gain_part = q_gain.shape[0]
    half = model // 2
    order = [2 * m for m in range(chips)] + [2 * m + 1 for m in range(chips)]
    slim = FF // wt_total

    def pick_blocks(values, places, width):
        return jnp.concatenate(
            [lax.dynamic_slice_in_dim(values, place * width, width, axis=1) for place in places],
            axis=1,
        )

    def to_relative(values):
        return pick_blocks(values, [wt_me ^ mask for mask in order], shard)

    def from_relative(values):
        masks = [wt_me ^ device for device in range(wt_total)]
        return pick_blocks(values, [mask // 2 + (mask % 2) * chips for mask in masks], shard)

    def by_chip(values):
        return pick_blocks(values, [chip ^ mask for mask in range(chips)], 2 * shard)

    small = jnp.concatenate(
        [
            w_router,
            attn_gain[:, None],
            ffn_gain[:, None],
            jnp.pad(q_gain, (0, shard - gain_part))[:, None],
            jnp.pad(k_gain, (0, shard - gain_part))[:, None],
        ],
        axis=1,
    )
    small = jnp.pad(small, ((0, 0), (0, LANES - small.shape[1])))
    qkv_here = jnp.concatenate(
        [
            lax.dynamic_slice_in_dim(w_qkv, kind * H * HD + seq_me * part, part, axis=1)
            for kind in range(3)
        ]
        + [small],
        axis=1,
    )
    token_ids = jnp.arange(experts, dtype=jnp.int32)
    routed_own = jnp.any(expert_routes[0][:, :, None] == token_ids[None, None, :], axis=1)
    tokens_sent = jnp.concatenate(
        [
            to_relative(tokens[0]),
            jnp.pad(routed_own.astype(BF), ((0, 0), (0, LANES - experts))),
        ],
        axis=1,
    )
    tokens_got = lax.all_gather(tokens_sent, "seq", axis=0, tiled=True)
    tokens_all = tokens_got[:, :model]
    routed = tokens_got[:, model : model + experts] > 0.5

    qkv_pieces = gather_chips(qkv_here, 0, chips)
    out_pieces = gather_chips(w_out, 1, chips)
    qkv_even = jnp.concatenate(qkv_pieces, axis=0)
    qkv_odd = swap(qkv_even, 1)
    out_even = jnp.concatenate(out_pieces, axis=0)
    out_odd = swap(out_even, 1)

    def columns_of(values, which):
        return jnp.concatenate(
            [
                values[:, (2 * j + which) * slim : (2 * j + which + 1) * slim]
                for j in range(wt_total)
            ],
            axis=1,
        )

    gate_ups = []
    downs = []
    ties = [qkv_pieces[1], qkv_pieces[2], out_pieces[1]]
    for e in range(local_experts):
        low_half = columns_of(w_gate_up[e], 0)
        high_half = columns_of(w_gate_up[e], 1)
        mine = jnp.where(first_core, low_half, high_half)
        others = swap(jnp.where(first_core, high_half, low_half), 1)
        pair = jnp.where(
            first_core,
            jnp.concatenate([mine, others], axis=0),
            jnp.concatenate([others, mine], axis=0),
        )
        down_own = w_down[e]
        pair, down_own, _ = lax.optimization_barrier((pair, down_own, tuple(ties)))
        pieces = gather_chips(pair, e % 2, chips)
        down_pieces = gather_chips(down_own, 1 - e % 2, chips)
        ties = [pieces[1], pieces[2]]
        gate_ups.append(jnp.concatenate(pieces, axis=0))
        down = jnp.zeros((FF // 2, model), BF)
        for mask in range(chips):
            down = lax.dynamic_update_slice_in_dim(
                down, down_pieces[mask], (chip ^ mask) * slim, axis=0
            )
        downs.append(down)

    grad_own, _ = lax.optimization_barrier((cotangent[0], tokens_got))
    grad_seq = lax.all_gather(grad_own, "seq", axis=0, tiled=True)
    grad_two = jnp.concatenate([grad_seq, swap(grad_seq, 1)], axis=0)

    small_relative = jnp.concatenate([qkv_even[:, cols:], qkv_odd[:, cols:]], axis=0)
    router = jnp.concatenate(
        [
            lax.dynamic_slice_in_dim(
                small_relative, (mask + (side ^ core) * chips) * shard, shard, axis=0
            )
            for mask in range(chips)
            for side in range(2)
        ],
        axis=0,
    )[:, :experts]
    picker = np.zeros((8, LANES), np.float32)
    for row in range(4):
        picker[row, experts + row] = 1.0
    gain_rows = nt(jnp.asarray(picker, BF), small_relative)
    gain_attn_relative = gain_rows[0]
    gain_rows = from_relative(gain_rows)
    gain_attn = gain_rows[0]
    gain_ffn = gain_rows[1]
    gain_query = gain_rows[2].reshape(wt_total, shard)[:, :gain_part].reshape(HD)
    gain_key = gain_rows[3].reshape(wt_total, shard)[:, :gain_part].reshape(HD)

    segments = segment_ids[0]
    same = segments[:, None] == segments[None, :]
    cosine, sine = rope_tables(length)
    normed_all, _ = normalize(tokens_all.astype(F32))
    hidden = (normed_all * gain_attn_relative).astype(BF)
    projected = nn(hidden[:, :half], qkv_even[:, :cols]) + nn(hidden[:, half:], qkv_odd[:, :cols])
    projected = projected.reshape(length, 3, heads, HD)
    normed_q, factor_q = normalize(projected[:, 0])
    normed_k, factor_k = normalize(projected[:, 1])
    queries = jnp.swapaxes(rotate(normed_q * gain_query, cosine, sine).astype(BF), 0, 1)
    keys = jnp.swapaxes(rotate(normed_k * gain_key, cosine, sine).astype(BF), 0, 1)
    values = jnp.swapaxes(projected[:, 2].astype(BF), 0, 1)
    scale = HD ** (-0.5)

    def bmm(left, right, dims):
        return lax.dot_general(left, right, (dims, ((0,), (0,))), preferred_element_type=F32)

    logits = jnp.where(same[None], bmm(queries, keys, ((2,), (2,))) * scale, NEG)
    powers = jnp.exp(logits - jnp.max(logits, axis=-1, keepdims=True))
    weights = powers / jnp.sum(powers, axis=-1, keepdims=True)
    weights_low = weights.astype(BF)
    attended = bmm(weights_low, values, ((2,), (1,))).astype(BF)
    merged = lax.all_to_all(
        jnp.swapaxes(attended, 0, 1), "seq", split_axis=0, concat_axis=1, tiled=True
    ).reshape(rows, H * HD)
    merged = to_relative(merged)

    inputs = tokens[0].astype(F32)
    residual = inputs + nn(merged[:, :half], out_even) + nn(merged[:, half:], out_odd)
    normed_f, factor_f = normalize(residual)
    hidden_own = (normed_f * gain_ffn).astype(BF)
    hidden_seq = lax.all_gather(by_chip(hidden_own), "seq", axis=0, tiled=True)
    hidden_two = jnp.concatenate([hidden_seq, swap(hidden_seq, 1)], axis=0)

    chances = jax.nn.softmax(nn(hidden_seq, router), axis=-1)
    picked = jnp.where(routed, chances, 0.0)
    picked_total = jnp.sum(picked, axis=1, keepdims=True)
    gates = picked / picked_total
    gates_seq = lax.dynamic_slice_in_dim(gates, seq_me * local_experts, local_experts, axis=1)
    gates_two = jnp.concatenate([gates_seq, swap(gates_seq, 1)], axis=0)

    grad_hidden_part = jnp.zeros((2 * length, model), F32)
    gate_grads = []
    wide_grads = []
    scaled_all = []
    for e in range(local_experts):
        gate = gates_two[:, e : e + 1]
        before = nn(hidden_two, gate_ups[e])
        gate_part = before[:, : FF // 2]
        up_part = before[:, FF // 2 :]
        sigmoid_gate = jax.nn.sigmoid(gate_part)
        silu_gate = gate_part * sigmoid_gate
        activated = silu_gate * up_part
        scaled = (gate * activated).astype(BF)
        grad_act = nt(grad_two, downs[e])
        gate_grads.append(jnp.sum(grad_act * activated, axis=1, keepdims=True))
        grad_act = grad_act * gate
        grad_gate = grad_act * up_part * sigmoid_gate * (1.0 + gate_part * (1.0 - sigmoid_gate))
        grad_up = grad_act * silu_gate
        grad_before = jnp.concatenate([grad_gate, grad_up], axis=-1).astype(BF)
        grad_hidden_part = grad_hidden_part + nt(grad_before, gate_ups[e])
        wide_grads.append(grad_before)
        scaled_all.append(scaled)

    gate_grad_two = jnp.concatenate(gate_grads, axis=1)
    gate_grad_part = gate_grad_two[:length] + swap(gate_grad_two[length:], 1)
    gate_high, gate_low = split_two(gate_grad_part)
    grad_hidden_low = (
        grad_hidden_part[:length] + swap(grad_hidden_part[length:].astype(BF), 1).astype(F32)
    ).astype(BF)

    def spread(values):
        wide = jnp.zeros((length, experts), BF)
        return lax.dynamic_update_slice(wide, values, (0, seq_me * local_experts))

    payload = jnp.concatenate([grad_hidden_low, spread(gate_high), spread(gate_low)], axis=1)
    returned = lax.psum_scatter(payload, "seq", scatter_dimension=0, tiled=True).astype(F32)
    gate_grad = returned[:, model : model + experts] + returned[:, model + experts :]
    wide_grads, scaled_all, _ = lax.optimization_barrier((wide_grads, scaled_all, payload))
    out_part = jnp.zeros((2 * length, model), F32)
    for e in range(local_experts):
        out_part = out_part + nn(scaled_all[e], downs[e])
    out_low = (out_part[:length] + swap(out_part[length:].astype(BF), 1).astype(F32)).astype(BF)
    out_low, _ = lax.optimization_barrier((out_low, returned))
    moe_out = lax.psum_scatter(out_low, "seq", scatter_dimension=0, tiled=True).astype(F32)
    output = (residual + moe_out).astype(BF)

    expert_parts = []
    for e in range(local_experts):
        parts = [
            tn(hidden_two[:, mask * 2 * shard : (mask + 1) * 2 * shard], wide_grads[e]).astype(BF)
            for mask in range(chips)
        ]
        down_grad = tn(scaled_all[e], grad_two).astype(BF)
        down_parts = [
            lax.dynamic_slice_in_dim(down_grad, (chip ^ mask) * slim, slim, axis=0)
            for mask in range(chips)
        ]
        expert_parts.append(
            (
                parts,
                send_first(parts, e % 2, chips),
                down_parts,
                send_first(down_parts, 1 - e % 2, chips),
            )
        )

    def finish_expert(e, anchor):
        group, _ = lax.optimization_barrier((expert_parts[e], anchor))
        parts, first, down_parts, down_first = group
        summed = scatter_chips(parts, e % 2, chips, first).astype(BF)
        down_row = scatter_chips(down_parts, 1 - e % 2, chips, down_first)
        kept = lax.dynamic_slice_in_dim(summed, core * shard, shard, axis=0)
        sent = lax.dynamic_slice_in_dim(summed, (1 - core) * shard, shard, axis=0)
        got = swap(sent, 1)
        low_half = jnp.where(first_core, kept, got)
        high_half = jnp.where(first_core, got, kept)
        gate_up_row = jnp.concatenate(
            [
                source[:, j * slim : (j + 1) * slim]
                for j in range(wt_total)
                for source in (low_half, high_half)
            ],
            axis=1,
        ).astype(F32)
        return gate_up_row, down_row

    def own(full):
        return lax.dynamic_slice_in_dim(full, seq_me * rows, rows, axis=0)

    chances_own = own(chances)
    gates_own = own(gates)
    inner_gate = jnp.sum(gate_grad * gates_own, axis=1, keepdims=True)
    grad_chances = jnp.where(routed_own, (gate_grad - inner_gate) / own(picked_total), 0.0)
    grad_logits = (
        chances_own
        * (grad_chances - jnp.sum(grad_chances * chances_own, axis=1, keepdims=True))
    ).astype(BF)
    grad_hidden = by_chip(returned[:, :model] + nt(grad_logits, router))
    router_grad = tn(
        to_relative(hidden_own), jnp.pad(grad_logits, ((0, 0), (0, LANES - experts)))
    )
    ffn_gain_grad = jnp.sum(grad_hidden * normed_f, axis=0)
    grad_residual = cotangent[0].astype(F32) + norm_back(
        grad_hidden * gain_ffn, normed_f, factor_f
    )
    grad_branch = grad_residual.astype(BF)
    grad_merged = jnp.concatenate([nt(grad_branch, out_even), nt(grad_branch, out_odd)], axis=1)
    grad_merged = from_relative(grad_merged.astype(BF)).reshape(rows, H, HD)
    grad_heads = jnp.swapaxes(
        lax.all_to_all(grad_merged, "seq", split_axis=1, concat_axis=0, tiled=True), 0, 1
    )

    def scatter_rows(left, right, route):
        sent = tn(left[:, half:], right).astype(BF)
        kept = (tn(left[:, :half], right) + swap(sent, 1).astype(F32)).astype(BF)
        parts = [kept[mask * shard : (mask + 1) * shard] for mask in range(chips)]
        return scatter_chips(parts, route, chips).astype(BF)

    out_grad = lax.psum(scatter_rows(merged, grad_branch, 1), "seq").astype(F32)

    grad_v = jnp.swapaxes(bmm(weights_low, grad_heads, ((1,), (1,))), 0, 1)
    grad_weights = bmm(grad_heads, values, ((2,), (2,)))
    inner = jnp.sum(weights * grad_weights, axis=-1, keepdims=True)
    grad_scores = (weights * (grad_weights - inner)).astype(BF)
    grad_q = jnp.swapaxes(bmm(grad_scores, keys, ((2,), (1,))), 0, 1) * scale
    grad_k = jnp.swapaxes(bmm(grad_scores, queries, ((1,), (1,))), 0, 1) * scale
    grad_q_normed = rotate(grad_q, cosine, -sine)
    grad_k_normed = rotate(grad_k, cosine, -sine)
    q_gain_grad = jnp.sum(grad_q_normed * normed_q, axis=(0, 1))
    k_gain_grad = jnp.sum(grad_k_normed * normed_k, axis=(0, 1))
    grad_q_raw = norm_back(grad_q_normed * gain_query, normed_q, factor_q)
    grad_k_raw = norm_back(grad_k_normed * gain_key, normed_k, factor_k)
    grads = [g.reshape(length, part).astype(BF) for g in (grad_q_raw, grad_k_raw, grad_v)]
    grad_projected = jnp.concatenate(grads, axis=1)
    grad_normed_part = jnp.concatenate(
        [nt(grad_projected, qkv_even[:, :cols]), nt(grad_projected, qkv_odd[:, :cols])], axis=1
    )
    attn_gain_grad = jnp.sum(grad_normed_part * normed_all, axis=0)
    grad_normed_own = lax.psum_scatter(
        grad_normed_part.astype(BF), "seq", scatter_dimension=0, tiled=True
    ).astype(F32)
    grad_normed_own = from_relative(grad_normed_own)
    normed_a, factor_a = normalize(inputs)
    tokens_grad = grad_residual + norm_back(grad_normed_own * gain_attn, normed_a, factor_a)

    def gain_line(vector):
        return jnp.pad(
            vector.reshape(wt_total, gain_part), ((0, 0), (0, shard - gain_part))
        ).reshape(model)

    lines = to_relative(
        jnp.stack([ffn_gain_grad, gain_line(q_gain_grad), gain_line(k_gain_grad)])
    )
    lines = jnp.concatenate([attn_gain_grad[None], lines, jnp.zeros((4, model), F32)], axis=0)
    small_grad = router_grad + tn(lines.astype(BF), jnp.asarray(picker, BF))
    small_sent = small_grad[half:].astype(BF)
    small_kept = (small_grad[:half] + swap(small_sent, 1).astype(F32)).astype(BF)
    small_sum = scatter_chips(
        [small_kept[mask * shard : (mask + 1) * shard] for mask in range(chips)], 1, chips
    ).astype(BF)
    value_sum = scatter_rows(hidden, grads[2], 0)
    query_sum = scatter_rows(hidden, grads[0], 1)
    key_sum = scatter_rows(hidden, grads[1], 0)
    collected_value = lax.all_gather(value_sum, "seq", axis=0)
    collected = lax.all_gather(
        jnp.concatenate([query_sum, key_sum, small_sum], axis=1), "seq", axis=0
    )
    qkv_out = jnp.concatenate(
        [collected[z, :, :part] for z in range(seq_total)]
        + [collected[z, :, part : 2 * part] for z in range(seq_total)]
        + [collected_value[z] for z in range(seq_total)],
        axis=1,
    ).astype(F32)
    small_out = jnp.sum(collected[:, :, 2 * part :].astype(F32), axis=0)
    anchors = [returned, grad_heads, grad_projected, grad_normed_part]
    expert_rows = [
        finish_expert(e, anchors[min(e * len(anchors) // local_experts, len(anchors) - 1)])
        for e in range(local_experts)
    ]
    gate_up_out = jnp.stack([row[0] for row in expert_rows])
    down_out = jnp.stack([row[1] for row in expert_rows])
    return (
        output[None],
        tokens_grad[None],
        qkv_out,
        out_grad,
        small_out[:, :experts],
        gate_up_out,
        down_out,
        small_out[:, experts],
        small_out[:, experts + 1],
        small_out[:gain_part, experts + 2],
        small_out[:gain_part, experts + 3],
    )


def solution(mesh):
    in_specs = (
        P("wt", "seq", None),
        P("wt", "seq", None),
        P("wt", None),
        P("wt", "seq", None),
        P("wt", None),
        P("wt", None),
        P("wt", None),
        P("seq", "wt", None),
        P("seq", "wt", None),
        P("wt"),
        P("wt"),
        P("wt"),
        P("wt"),
    )
    out_specs = (
        P("wt", "seq", None),
        P("wt", "seq", None),
        P("wt", None),
        P("wt", None),
        P("wt", None),
        P("seq", "wt", None),
        P("seq", "wt", None),
        P("wt"),
        P("wt"),
        P("wt"),
        P("wt"),
    )
    return jax.shard_map(body, mesh=mesh, in_specs=in_specs, out_specs=out_specs, check_vma=False)
```

```python
import jax
import jax.numpy as jnp
import numpy as np
from jax import lax
from jax.sharding import PartitionSpec as P


H = 16
HD = 128
FF = 1024

EPS = 1e-06
THETA = 50000.0
NEG = -1e30
LANES = 128
BF = jnp.bfloat16
F32 = jnp.float32


def normalize(values):
    factor = lax.rsqrt(jnp.mean(values * values, axis=-1, keepdims=True) + EPS)
    return (values * factor, factor)


def norm_back(grad_normed, normed_values, factor):
    return factor * (
        grad_normed - normed_values * jnp.mean(grad_normed * normed_values, axis=-1, keepdims=True)
    )


def rope_tables(length):
    half = HD // 2
    freq = THETA ** (-jnp.arange(half, dtype=F32) * 2.0 / HD)
    angle = jnp.arange(length, dtype=F32)[:, None] * freq[None, :]
    return jnp.cos(angle)[:, None, :], jnp.sin(angle)[:, None, :]


def rotate(values, cosine, sine):
    half = values.shape[-1] // 2
    first = values[..., :half]
    second = values[..., half:]
    return jnp.concatenate(
        [first * cosine - second * sine, second * cosine + first * sine], axis=-1
    )


def dot(left, right, dims):
    return lax.dot_general(left, right, (dims, ((), ())), preferred_element_type=F32)


def nn(left, right):
    return dot(left, right, ((1,), (0,)))


def nt(left, right):
    return dot(left, right, ((1,), (1,)))


def tn(left, right):
    return dot(left, right, ((0,), (0,)))


def split_two(values):
    high = values.astype(BF)
    low = (values - high.astype(F32)).astype(BF)
    return high, low


def swap(values, bit):
    total = lax.axis_size("wt")
    return lax.ppermute(values, "wt", [(i, i ^ bit) for i in range(total)])


def bits_of(chips, route):
    bits = []
    while 1 << len(bits) < chips:
        bits.append(1 << len(bits))
    return bits[::-1] if route else bits


def zero_of(anchor):
    return anchor[(0,) * anchor.ndim].astype(F32) * 0.0


def later(values, anchor):
    return (values.astype(F32) + zero_of(anchor)).astype(values.dtype)


def first_gather(own, route, chips):
    bits = bits_of(chips, route)
    return {bit: swap(own, 2 * bit) for bit in bits}


def rest_gather(own, direct, route, chips, anchor, use):
    pieces = {0: own}
    handed = {0}
    for bit in bits_of(chips, route):
        for mask in list(pieces):
            if mask:
                if mask not in handed:
                    pieces[mask] = later(pieces[mask], anchor)
                    handed.add(mask)
                pieces[mask ^ bit] = swap(pieces[mask], 2 * bit)
            else:
                pieces[bit] = direct[bit]
    return [
        pieces[mask] if mask in handed else later(pieces[mask], use) for mask in range(chips)
    ]


def gather_chips(own, route, chips):
    bits = bits_of(chips, route)
    pieces = {0: own}
    for bit in bits:
        for mask in list(pieces):
            pieces[mask ^ bit] = swap(pieces[mask], 2 * bit)
    return [pieces[mask] for mask in range(chips)]


def send_first(parts, route, chips):
    bit = bits_of(chips, route)[0]
    return {mask: swap(parts[mask], 2 * bit) for mask in range(chips) if mask & bit}


def scatter_chips(parts, route, chips, first=None, anchor=None):
    bits = bits_of(chips, route)
    held = dict(enumerate(parts))
    if first is None:
        first = send_first(parts, route, chips)
    zero = 0.0 if anchor is None else zero_of(anchor)
    for place, bit in enumerate(bits):
        for mask in [m for m in held if m & bit]:
            sent = held.pop(mask)
            arrived = swap(sent, 2 * bit) if place else first[mask]
            total = held[mask ^ bit].astype(F32) + arrived.astype(F32) + zero
            rest = [b for b in bits[place + 1 :] if (mask ^ bit) & b]
            held[mask ^ bit] = total.astype(BF) if rest else total
    return held[0]


def body(
    tokens,
    cotangent,
    segment_ids,
    expert_routes,
    w_qkv,
    w_out,
    w_router,
    w_gate_up,
    w_down,
    attn_gain,
    ffn_gain,
    q_gain,
    k_gain,
):
    seq_total = lax.axis_size("seq")
    wt_total = lax.axis_size("wt")
    seq_me = lax.axis_index("seq")
    wt_me = lax.axis_index("wt")
    core = wt_me % 2
    chip = wt_me // 2
    chips = wt_total // 2
    first_core = core == 0
    rows = tokens.shape[1]
    model = tokens.shape[2]
    length = rows * seq_total
    shard = model // wt_total
    local_experts = w_gate_up.shape[0]
    experts = w_router.shape[1]
    heads = H // seq_total
    part = heads * HD
    cols = 3 * part
    gain_part = q_gain.shape[0]
    half = model // 2
    order = [2 * m for m in range(chips)] + [2 * m + 1 for m in range(chips)]
    slim = FF // wt_total

    def pick_blocks(values, places, width):
        return jnp.concatenate(
            [lax.dynamic_slice_in_dim(values, place * width, width, axis=1) for place in places],
            axis=1,
        )

    def to_relative(values):
        return pick_blocks(values, [wt_me ^ mask for mask in order], shard)

    def from_relative(values):
        masks = [wt_me ^ device for device in range(wt_total)]
        return pick_blocks(values, [mask // 2 + (mask % 2) * chips for mask in masks], shard)

    def by_chip(values):
        return pick_blocks(values, [chip ^ mask for mask in range(chips)], 2 * shard)

    small = jnp.concatenate(
        [
            w_router,
            attn_gain[:, None],
            ffn_gain[:, None],
            jnp.pad(q_gain, (0, shard - gain_part))[:, None],
            jnp.pad(k_gain, (0, shard - gain_part))[:, None],
        ],
        axis=1,
    )
    small = jnp.pad(small, ((0, 0), (0, LANES - small.shape[1])))
    qkv_here = jnp.concatenate(
        [
            lax.dynamic_slice_in_dim(w_qkv, kind * H * HD + seq_me * part, part, axis=1)
            for kind in range(3)
        ]
        + [small],
        axis=1,
    )
    token_ids = jnp.arange(experts, dtype=jnp.int32)
    routed_own = jnp.any(expert_routes[0][:, :, None] == token_ids[None, None, :], axis=1)
    tokens_sent = jnp.concatenate(
        [
            to_relative(tokens[0]),
            jnp.pad(routed_own.astype(BF), ((0, 0), (0, LANES - experts))),
        ],
        axis=1,
    )
    tokens_got = lax.all_gather(tokens_sent, "seq", axis=0, tiled=True)
    tokens_all = tokens_got[:, :model]
    routed = tokens_got[:, model : model + experts] > 0.5

    qkv_pieces = gather_chips(qkv_here, 0, chips)
    out_pieces = gather_chips(w_out, 1, chips)
    qkv_blocks = qkv_pieces + [swap(piece, 1) for piece in qkv_pieces]
    out_even = jnp.concatenate(out_pieces, axis=0)
    out_odd = swap(out_even, 1)

    def columns_of(values, which):
        return jnp.concatenate(
            [
                values[:, (2 * j + which) * slim : (2 * j + which + 1) * slim]
                for j in range(wt_total)
            ],
            axis=1,
        )

    pairs = []
    pairs_direct = []
    downs_own = []
    downs_direct = []

    def send_expert(e, anchor):
        zero = zero_of(anchor)
        low_half = columns_of(w_gate_up[e], 0)
        high_half = columns_of(w_gate_up[e], 1)
        mine = jnp.where(first_core, low_half, high_half)
        others = swap(jnp.where(first_core, high_half, low_half), 1)
        pair = jnp.where(
            first_core,
            jnp.concatenate([mine, others], axis=0),
            jnp.concatenate([others, mine], axis=0),
        )
        pair = (pair.astype(F32) + zero).astype(BF)
        down_own = (w_down[e].astype(F32) + zero).astype(BF)
        pairs.append(pair)
        downs_own.append(down_own)
        pairs_direct.append(first_gather(pair, e % 2, chips))
        downs_direct.append(first_gather(down_own, 1 - e % 2, chips))

    def expert_weights(e, anchor, use):
        pieces = rest_gather(pairs[e], pairs_direct[e], e % 2, chips, anchor, use)
        down_pieces = rest_gather(
            downs_own[e], downs_direct[e], 1 - e % 2, chips, anchor, use
        )
        down = jnp.zeros((FF // 2, model), BF)
        for mask in range(chips):
            down = lax.dynamic_update_slice_in_dim(
                down, down_pieces[mask], (chip ^ mask) * slim, axis=0
            )
        return jnp.concatenate(pieces, axis=0), down

    starts = [qkv_pieces[-1], qkv_pieces[-1], out_pieces[1]]
    for e in range(min(local_experts, 3)):
        send_expert(e, starts[e])

    grad_own = later(cotangent[0], tokens_got)
    grad_seq = lax.all_gather(grad_own, "seq", axis=0, tiled=True)
    grad_two = jnp.concatenate([grad_seq, swap(grad_seq, 1)], axis=0)

    small_relative = jnp.concatenate([block[:, cols:] for block in qkv_blocks], axis=0)
    router = jnp.concatenate(
        [
            lax.dynamic_slice_in_dim(
                small_relative, (mask + (side ^ core) * chips) * shard, shard, axis=0
            )
            for mask in range(chips)
            for side in range(2)
        ],
        axis=0,
    )[:, :experts]
    picker = np.zeros((8, LANES), np.float32)
    for row in range(4):
        picker[row, experts + row] = 1.0
    gain_rows = nt(jnp.asarray(picker, BF), small_relative)
    gain_attn_relative = gain_rows[0]
    gain_rows = from_relative(gain_rows)
    gain_attn = gain_rows[0]
    gain_ffn = gain_rows[1]
    gain_query = gain_rows[2].reshape(wt_total, shard)[:, :gain_part].reshape(HD)
    gain_key = gain_rows[3].reshape(wt_total, shard)[:, :gain_part].reshape(HD)

    segments = segment_ids[0]
    same = segments[:, None] == segments[None, :]
    cosine, sine = rope_tables(length)
    normed_all, _ = normalize(tokens_all.astype(F32))
    hidden = (normed_all * gain_attn_relative).astype(BF)
    qkv_full = jnp.zeros((model, cols), BF)
    for place, block in enumerate(qkv_blocks):
        qkv_full = lax.dynamic_update_slice_in_dim(
            qkv_full, block[:, :cols], place * shard, axis=0
        )
    projected = nn(hidden, qkv_full)
    projected = projected.reshape(length, 3, heads, HD)
    normed_q, factor_q = normalize(projected[:, 0])
    normed_k, factor_k = normalize(projected[:, 1])
    queries = jnp.swapaxes(rotate(normed_q * gain_query, cosine, sine).astype(BF), 0, 1)
    keys = jnp.swapaxes(rotate(normed_k * gain_key, cosine, sine).astype(BF), 0, 1)
    values = jnp.swapaxes(projected[:, 2].astype(BF), 0, 1)
    scale = HD ** (-0.5)

    def bmm(left, right, dims):
        return lax.dot_general(left, right, (dims, ((0,), (0,))), preferred_element_type=F32)

    logits = jnp.where(same[None], bmm(queries, keys, ((2,), (2,))) * scale, NEG)
    powers = jnp.exp(logits - jnp.max(logits, axis=-1, keepdims=True))
    weights = powers / jnp.sum(powers, axis=-1, keepdims=True)
    weights_low = weights.astype(BF)
    attended = bmm(weights_low, values, ((2,), (1,))).astype(BF)
    merged = lax.all_to_all(
        jnp.swapaxes(attended, 0, 1), "seq", split_axis=0, concat_axis=1, tiled=True
    ).reshape(rows, H * HD)
    for e in range(min(local_experts, 3), local_experts):
        send_expert(e, attended)
    merged = to_relative(merged)

    inputs = tokens[0].astype(F32)
    residual = inputs + nn(merged[:, :half], out_even) + nn(merged[:, half:], out_odd)
    normed_f, factor_f = normalize(residual)
    hidden_own = (normed_f * gain_ffn).astype(BF)
    hidden_sent = by_chip(hidden_own)
    hidden_seq = lax.all_gather(hidden_sent, "seq", axis=0, tiled=True)
    forward_marks = [attended, merged, hidden_own]
    use_marks = [hidden_own, hidden_own]
    gate_ups = []
    downs = []
    for e in range(min(local_experts, 2)):
        gate_up, down = expert_weights(e, forward_marks[e], use_marks[e])
        gate_ups.append(gate_up)
        downs.append(down)
    hidden_two = jnp.concatenate([hidden_seq, swap(hidden_seq, 1)], axis=0)

    chances = jax.nn.softmax(nn(hidden_seq, router), axis=-1)
    picked = jnp.where(routed, chances, 0.0)
    picked_total = jnp.sum(picked, axis=1, keepdims=True)
    gates = picked / picked_total
    gates_seq = lax.dynamic_slice_in_dim(gates, seq_me * local_experts, local_experts, axis=1)
    gates_two = jnp.concatenate([gates_seq, swap(gates_seq, 1)], axis=0)

    grad_hidden_part = jnp.zeros((2 * length, model), F32)
    gate_grads = []
    wide_grads = []
    scaled_all = []
    for e in range(local_experts):
        gate = gates_two[:, e : e + 1]
        if e >= 2:
            mark = hidden_seq if e == 2 else wide_grads[e - 3]
            gate_up, down = expert_weights(e, mark, wide_grads[e - 2])
            gate_ups.append(gate_up)
            downs.append(down)
        before = nn(hidden_two, gate_ups[e])
        gate_part = before[:, : FF // 2]
        up_part = before[:, FF // 2 :]
        sigmoid_gate = jax.nn.sigmoid(gate_part)
        silu_gate = gate_part * sigmoid_gate
        activated = silu_gate * up_part
        scaled = (gate * activated).astype(BF)
        grad_act = nt(grad_two, downs[e])
        gate_grads.append(jnp.sum(grad_act * activated, axis=1, keepdims=True))
        grad_act = grad_act * gate
        grad_gate = grad_act * up_part * sigmoid_gate * (1.0 + gate_part * (1.0 - sigmoid_gate))
        grad_up = grad_act * silu_gate
        grad_before = jnp.concatenate([grad_gate, grad_up], axis=-1).astype(BF)
        grad_hidden_part = grad_hidden_part + nt(grad_before, gate_ups[e])
        wide_grads.append(grad_before)
        scaled_all.append(scaled)

    gate_grad_two = jnp.concatenate(gate_grads, axis=1)
    gate_grad_part = gate_grad_two[:length] + swap(gate_grad_two[length:], 1)
    gate_high, gate_low = split_two(gate_grad_part)
    grad_hidden_low = (
        grad_hidden_part[:length] + swap(grad_hidden_part[length:].astype(BF), 1).astype(F32)
    ).astype(BF)

    def spread(values):
        wide = jnp.zeros((length, experts), BF)
        return lax.dynamic_update_slice(wide, values, (0, seq_me * local_experts))

    payload = jnp.concatenate([grad_hidden_low, spread(gate_high), spread(gate_low)], axis=1)
    returned = lax.psum_scatter(payload, "seq", scatter_dimension=0, tiled=True)
    returned = returned.astype(F32)
    gate_grad = returned[:, model : model + experts] + returned[:, model + experts :]
    expert_parts = []

    def start_expert(e, anchor):
        wide = later(wide_grads[e], anchor)
        scaled = later(scaled_all[e], anchor)
        parts = [
            tn(hidden_two[:, mask * 2 * shard : (mask + 1) * 2 * shard], wide).astype(BF)
            for mask in range(chips)
        ]
        down_grad = tn(scaled, grad_two).astype(BF)
        down_parts = [
            lax.dynamic_slice_in_dim(down_grad, (chip ^ mask) * slim, slim, axis=0)
            for mask in range(chips)
        ]
        sent = send_first(parts, e % 2, chips)
        down_sent = send_first(down_parts, 1 - e % 2, chips)
        expert_parts.append((parts, sent, down_parts, down_sent))

    start_expert(0, payload)
    start_expert(1, payload)

    def finish_expert(e, anchor):
        parts, first, down_parts, down_first = expert_parts[e]
        summed = scatter_chips(parts, e % 2, chips, first, anchor).astype(BF)
        down_row = scatter_chips(down_parts, 1 - e % 2, chips, down_first, anchor)
        kept = lax.dynamic_slice_in_dim(summed, core * shard, shard, axis=0)
        sent = lax.dynamic_slice_in_dim(summed, (1 - core) * shard, shard, axis=0)
        got = swap(sent, 1)
        low_half = jnp.where(first_core, kept, got)
        high_half = jnp.where(first_core, got, kept)
        gate_up_row = jnp.concatenate(
            [
                source[:, j * slim : (j + 1) * slim]
                for j in range(wt_total)
                for source in (low_half, high_half)
            ],
            axis=1,
        ).astype(F32)
        return gate_up_row, down_row

    def own(full):
        return lax.dynamic_slice_in_dim(full, seq_me * rows, rows, axis=0)

    chances_own = own(chances)
    gates_own = own(gates)
    inner_gate = jnp.sum(gate_grad * gates_own, axis=1, keepdims=True)
    grad_chances = jnp.where(routed_own, (gate_grad - inner_gate) / own(picked_total), 0.0)
    grad_logits = (
        chances_own
        * (grad_chances - jnp.sum(grad_chances * chances_own, axis=1, keepdims=True))
    ).astype(BF)
    grad_hidden = by_chip(returned[:, :model] + nt(grad_logits, router))
    router_grad = tn(
        to_relative(hidden_own), jnp.pad(grad_logits, ((0, 0), (0, LANES - experts)))
    )
    ffn_gain_grad = jnp.sum(grad_hidden * normed_f, axis=0)
    grad_residual = cotangent[0].astype(F32) + norm_back(
        grad_hidden * gain_ffn, normed_f, factor_f
    )
    grad_branch = grad_residual.astype(BF)
    grad_merged = jnp.concatenate(
        [nt(grad_branch, out_even), nt(grad_branch, out_odd)], axis=1
    )
    grad_merged = from_relative(grad_merged.astype(BF))
    for e in range(2, min(local_experts, 3)):
        start_expert(e, grad_merged)
    grad_merged = grad_merged.reshape(rows, H, HD)
    grad_heads = jnp.swapaxes(
        lax.all_to_all(grad_merged, "seq", split_axis=1, concat_axis=0, tiled=True), 0, 1
    )

    scaled_out = [later(scaled, grad_heads) for scaled in scaled_all]
    out_part = jnp.zeros((2 * length, model), F32)
    for e in range(local_experts):
        out_part = out_part + nn(scaled_out[e], downs[e])
    out_other = swap(out_part[length:].astype(BF), 1)
    out_low = (out_part[:length] + out_other.astype(F32)).astype(BF)
    moe_out = lax.psum_scatter(out_low, "seq", scatter_dimension=0, tiled=True)
    moe_out = moe_out.astype(F32)

    def scatter_rows(left, right, route):
        sent = tn(left[:, half:], right).astype(BF)
        other = swap(sent, 1)
        kept = (tn(left[:, :half], right) + other.astype(F32)).astype(BF)
        parts = [kept[mask * shard : (mask + 1) * shard] for mask in range(chips)]
        first = send_first(parts, route, chips)
        return scatter_chips(parts, route, chips, first).astype(BF)

    out_sum = scatter_rows(later(merged, grad_merged), grad_branch, 1)

    out_grad = lax.psum(out_sum, "seq")
    out_grad = out_grad.astype(F32)

    grad_v = jnp.swapaxes(bmm(weights_low, grad_heads, ((1,), (1,))), 0, 1)
    grad_weights = bmm(grad_heads, values, ((2,), (2,)))
    inner = jnp.sum(weights * grad_weights, axis=-1, keepdims=True)
    grad_scores = (weights * (grad_weights - inner)).astype(BF)
    grad_q = jnp.swapaxes(bmm(grad_scores, keys, ((2,), (1,))), 0, 1) * scale
    grad_k = jnp.swapaxes(bmm(grad_scores, queries, ((1,), (1,))), 0, 1) * scale
    grad_q_normed = rotate(grad_q, cosine, -sine)
    grad_k_normed = rotate(grad_k, cosine, -sine)
    q_gain_grad = jnp.sum(grad_q_normed * normed_q, axis=(0, 1))
    k_gain_grad = jnp.sum(grad_k_normed * normed_k, axis=(0, 1))
    grad_q_raw = norm_back(grad_q_normed * gain_query, normed_q, factor_q)
    grad_k_raw = norm_back(grad_k_normed * gain_key, normed_k, factor_k)
    grads = [g.reshape(length, part).astype(BF) for g in (grad_q_raw, grad_k_raw, grad_v)]
    grad_projected = jnp.concatenate(grads, axis=1)
    grad_normed_part = nt(grad_projected, qkv_full)
    attn_gain_grad = jnp.sum(grad_normed_part * normed_all, axis=0)
    grad_normed_low = grad_normed_part.astype(BF)
    grad_normed_own = lax.psum_scatter(
        grad_normed_low, "seq", scatter_dimension=0, tiled=True
    )
    grad_normed_own = grad_normed_own.astype(F32)
    grad_normed_own = from_relative(grad_normed_own)
    normed_a, factor_a = normalize(inputs)
    tokens_grad = grad_residual + norm_back(grad_normed_own * gain_attn, normed_a, factor_a)

    def gain_line(vector):
        return jnp.pad(
            vector.reshape(wt_total, gain_part), ((0, 0), (0, shard - gain_part))
        ).reshape(model)

    lines = to_relative(
        jnp.stack([ffn_gain_grad, gain_line(q_gain_grad), gain_line(k_gain_grad)])
    )
    lines = jnp.concatenate([attn_gain_grad[None], lines, jnp.zeros((4, model), F32)], axis=0)
    small_grad = router_grad + tn(lines.astype(BF), jnp.asarray(picker, BF))
    small_sent = small_grad[half:].astype(BF)
    small_kept = (small_grad[:half] + swap(small_sent, 1).astype(F32)).astype(BF)
    small_sum = scatter_chips(
        [small_kept[mask * shard : (mask + 1) * shard] for mask in range(chips)], 1, chips
    ).astype(BF)
    for e in range(3, local_experts):
        start_expert(e, grad_normed_low)
    value_sum = scatter_rows(hidden, grads[2], 0)
    query_sum = scatter_rows(hidden, grads[0], 1)
    key_sum = scatter_rows(hidden, grads[1], 0)
    collected_value = lax.all_gather(value_sum, "seq", axis=0)
    collected = lax.all_gather(
        jnp.concatenate([query_sum, key_sum, small_sum], axis=1), "seq", axis=0
    )
    qkv_out = jnp.concatenate(
        [collected[z, :, :part] for z in range(seq_total)]
        + [collected[z, :, part : 2 * part] for z in range(seq_total)]
        + [collected_value[z] for z in range(seq_total)],
        axis=1,
    ).astype(F32)
    small_out = jnp.sum(collected[:, :, 2 * part :].astype(F32), axis=0)
    anchors = [grad_heads, grad_projected, query_sum, key_sum]
    expert_rows = [
        finish_expert(e, anchors[min(e * len(anchors) // local_experts, len(anchors) - 1)])
        for e in range(local_experts)
    ]
    gate_up_out = jnp.stack([row[0] for row in expert_rows])
    down_out = jnp.stack([row[1] for row in expert_rows])
    output = (residual + moe_out + zero_of(grad_projected)).astype(BF)
    return (
        output[None],
        tokens_grad[None],
        qkv_out,
        out_grad,
        small_out[:, :experts],
        gate_up_out,
        down_out,
        small_out[:, experts],
        small_out[:, experts + 1],
        small_out[:gain_part, experts + 2],
        small_out[:gain_part, experts + 3],
    )


def solution(mesh):
    in_specs = (
        P("wt", "seq", None),
        P("wt", "seq", None),
        P("wt", None),
        P("wt", "seq", None),
        P("wt", None),
        P("wt", None),
        P("wt", None),
        P("seq", "wt", None),
        P("seq", "wt", None),
        P("wt"),
        P("wt"),
        P("wt"),
        P("wt"),
    )
    out_specs = (
        P("wt", "seq", None),
        P("wt", "seq", None),
        P("wt", None),
        P("wt", None),
        P("wt", None),
        P("seq", "wt", None),
        P("seq", "wt", None),
        P("wt"),
        P("wt"),
        P("wt"),
        P("wt"),
    )

    return jax.shard_map(body, mesh=mesh, in_specs=in_specs, out_specs=out_specs, check_vma=False)
```

```python
import jax
import jax.numpy as jnp
import numpy as np
from jax import lax
from jax.sharding import PartitionSpec as P


H = 16
HD = 128
FF = 1024

EPS = 1e-06
THETA = 50000.0
NEG = -1e30
LANES = 128
BF = jnp.bfloat16
F32 = jnp.float32


def normalize(values):
    factor = lax.rsqrt(jnp.mean(values * values, axis=-1, keepdims=True) + EPS)
    return (values * factor, factor)


def norm_back(grad_normed, normed_values, factor):
    return factor * (
        grad_normed - normed_values * jnp.mean(grad_normed * normed_values, axis=-1, keepdims=True)
    )


def rope_tables(length):
    half = HD // 2
    freq = THETA ** (-jnp.arange(half, dtype=F32) * 2.0 / HD)
    angle = jnp.arange(length, dtype=F32)[:, None] * freq[None, :]
    return jnp.cos(angle)[:, None, :], jnp.sin(angle)[:, None, :]


def rotate(values, cosine, sine):
    half = values.shape[-1] // 2
    first = values[..., :half]
    second = values[..., half:]
    return jnp.concatenate(
        [first * cosine - second * sine, second * cosine + first * sine], axis=-1
    )


def dot(left, right, dims):
    return lax.dot_general(left, right, (dims, ((), ())), preferred_element_type=F32)


def nn(left, right):
    return dot(left, right, ((1,), (0,)))


def nt(left, right):
    return dot(left, right, ((1,), (1,)))


def tn(left, right):
    return dot(left, right, ((0,), (0,)))


def split_two(values):
    high = values.astype(BF)
    low = (values - high.astype(F32)).astype(BF)
    return high, low


def swap(values, bit):
    total = lax.axis_size("wt")
    return lax.ppermute(values, "wt", [(i, i ^ bit) for i in range(total)])


def bits_of(chips, route):
    bits = []
    while 1 << len(bits) < chips:
        bits.append(1 << len(bits))
    return bits[::-1] if route else bits


def zero_of(anchor):
    return anchor[(0,) * anchor.ndim].astype(F32) * 0.0


def later(values, anchor):
    return (values.astype(F32) + zero_of(anchor)).astype(values.dtype)


def first_gather(own, route, chips):
    bits = bits_of(chips, route)
    return {bit: swap(own, 2 * bit) for bit in bits}


def rest_gather(own, direct, route, chips, anchor, use):
    pieces = {0: own}
    handed = {0}
    for bit in bits_of(chips, route):
        for mask in list(pieces):
            if mask:
                if mask not in handed:
                    pieces[mask] = later(pieces[mask], anchor)
                    handed.add(mask)
                pieces[mask ^ bit] = swap(pieces[mask], 2 * bit)
            else:
                pieces[bit] = direct[bit]
    return [
        pieces[mask] if mask in handed else later(pieces[mask], use) for mask in range(chips)
    ]


def gather_chips(own, route, chips):
    bits = bits_of(chips, route)
    pieces = {0: own}
    for bit in bits:
        for mask in list(pieces):
            pieces[mask ^ bit] = swap(pieces[mask], 2 * bit)
    return [pieces[mask] for mask in range(chips)]


def send_first(parts, route, chips):
    bit = bits_of(chips, route)[0]
    return {mask: swap(parts[mask], 2 * bit) for mask in range(chips) if mask & bit}


def scatter_chips(parts, route, chips, first=None, anchor=None):
    bits = bits_of(chips, route)
    held = dict(enumerate(parts))
    if first is None:
        first = send_first(parts, route, chips)
    zero = 0.0 if anchor is None else zero_of(anchor)
    for place, bit in enumerate(bits):
        for mask in [m for m in held if m & bit]:
            sent = held.pop(mask)
            arrived = swap(sent, 2 * bit) if place else first[mask]
            total = held[mask ^ bit].astype(F32) + arrived.astype(F32) + zero
            rest = [b for b in bits[place + 1 :] if (mask ^ bit) & b]
            held[mask ^ bit] = total.astype(BF) if rest else total
    return held[0]


def body(
    tokens,
    cotangent,
    segment_ids,
    expert_routes,
    w_qkv,
    w_out,
    w_router,
    w_gate_up,
    w_down,
    attn_gain,
    ffn_gain,
    q_gain,
    k_gain,
):
    seq_total = lax.axis_size("seq")
    wt_total = lax.axis_size("wt")
    seq_me = lax.axis_index("seq")
    wt_me = lax.axis_index("wt")
    core = wt_me % 2
    chip = wt_me // 2
    chips = wt_total // 2
    first_core = core == 0
    rows = tokens.shape[1]
    model = tokens.shape[2]
    length = rows * seq_total
    shard = model // wt_total
    local_experts = w_gate_up.shape[0]
    experts = w_router.shape[1]
    heads = H // seq_total
    part = heads * HD
    cols = 3 * part
    gain_part = q_gain.shape[0]
    half = model // 2
    order = [2 * m for m in range(chips)] + [2 * m + 1 for m in range(chips)]
    slim = FF // wt_total

    def pick_blocks(values, places, width):
        return jnp.concatenate(
            [lax.dynamic_slice_in_dim(values, place * width, width, axis=1) for place in places],
            axis=1,
        )

    def to_relative(values):
        return pick_blocks(values, [wt_me ^ mask for mask in order], shard)

    def from_relative(values):
        masks = [wt_me ^ device for device in range(wt_total)]
        return pick_blocks(values, [mask // 2 + (mask % 2) * chips for mask in masks], shard)

    def by_chip(values):
        return pick_blocks(values, [chip ^ mask for mask in range(chips)], 2 * shard)

    small = jnp.concatenate(
        [
            w_router,
            attn_gain[:, None],
            ffn_gain[:, None],
            jnp.pad(q_gain, (0, shard - gain_part))[:, None],
            jnp.pad(k_gain, (0, shard - gain_part))[:, None],
        ],
        axis=1,
    )
    small = jnp.pad(small, ((0, 0), (0, LANES - small.shape[1])))
    qkv_here = jnp.concatenate(
        [
            lax.dynamic_slice_in_dim(w_qkv, kind * H * HD + seq_me * part, part, axis=1)
            for kind in range(3)
        ]
        + [small],
        axis=1,
    )
    token_ids = jnp.arange(experts, dtype=jnp.int32)
    routed_own = jnp.any(expert_routes[0][:, :, None] == token_ids[None, None, :], axis=1)
    tokens_sent = jnp.concatenate(
        [
            to_relative(tokens[0]),
            jnp.pad(routed_own.astype(BF), ((0, 0), (0, LANES - experts))),
        ],
        axis=1,
    )
    tokens_got = lax.all_gather(tokens_sent, "seq", axis=0, tiled=True)
    tokens_all = tokens_got[:, :model]
    routed = tokens_got[:, model : model + experts] > 0.5

    qkv_pieces = gather_chips(qkv_here, 0, chips)
    out_pieces = gather_chips(w_out, 1, chips)
    qkv_blocks = qkv_pieces + [swap(piece, 1) for piece in qkv_pieces]
    out_even = jnp.concatenate(out_pieces, axis=0)
    out_odd = swap(out_even, 1)

    def columns_of(values, which):
        return jnp.concatenate(
            [
                values[:, (2 * j + which) * slim : (2 * j + which + 1) * slim]
                for j in range(wt_total)
            ],
            axis=1,
        )

    pairs = []
    pairs_direct = []
    downs_own = []
    downs_direct = []

    def send_expert(e, anchor):
        zero = zero_of(anchor)
        low_half = columns_of(w_gate_up[e], 0)
        high_half = columns_of(w_gate_up[e], 1)
        mine = jnp.where(first_core, low_half, high_half)
        others = swap(jnp.where(first_core, high_half, low_half), 1)
        pair = jnp.where(
            first_core,
            jnp.concatenate([mine, others], axis=0),
            jnp.concatenate([others, mine], axis=0),
        )
        pair = (pair.astype(F32) + zero).astype(BF)
        down_own = (w_down[e].astype(F32) + zero).astype(BF)
        pairs.append(pair)
        downs_own.append(down_own)
        pairs_direct.append(first_gather(pair, e % 2, chips))
        downs_direct.append(first_gather(down_own, 1 - e % 2, chips))

    def expert_weights(e, anchor, use):
        pieces = rest_gather(pairs[e], pairs_direct[e], e % 2, chips, anchor, use)
        down_pieces = rest_gather(
            downs_own[e], downs_direct[e], 1 - e % 2, chips, anchor, use
        )
        down = jnp.zeros((FF // 2, model), BF)
        for mask in range(chips):
            down = lax.dynamic_update_slice_in_dim(
                down, down_pieces[mask], (chip ^ mask) * slim, axis=0
            )
        return jnp.concatenate(pieces, axis=0), down

    starts = [qkv_pieces[-1], qkv_pieces[-1], out_pieces[1]]
    for e in range(min(local_experts, 3)):
        send_expert(e, starts[e])

    grad_own = later(cotangent[0], tokens_got)
    grad_seq = lax.all_gather(grad_own, "seq", axis=0, tiled=True)
    grad_two = jnp.concatenate([grad_seq, swap(grad_seq, 1)], axis=0)

    small_relative = jnp.concatenate([block[:, cols:] for block in qkv_blocks], axis=0)
    router = jnp.concatenate(
        [
            lax.dynamic_slice_in_dim(
                small_relative, (mask + (side ^ core) * chips) * shard, shard, axis=0
            )
            for mask in range(chips)
            for side in range(2)
        ],
        axis=0,
    )[:, :experts]
    picker = np.zeros((8, LANES), np.float32)
    for row in range(4):
        picker[row, experts + row] = 1.0
    gain_rows = nt(jnp.asarray(picker, BF), small_relative)
    gain_attn_relative = gain_rows[0]
    gain_rows = from_relative(gain_rows)
    gain_attn = gain_rows[0]
    gain_ffn = gain_rows[1]
    gain_query = gain_rows[2].reshape(wt_total, shard)[:, :gain_part].reshape(HD)
    gain_key = gain_rows[3].reshape(wt_total, shard)[:, :gain_part].reshape(HD)

    segments = segment_ids[0]
    same = segments[:, None] == segments[None, :]
    cosine, sine = rope_tables(length)
    normed_all, _ = normalize(tokens_all.astype(F32))
    hidden = (normed_all * gain_attn_relative).astype(BF)
    qkv_full = jnp.zeros((model, cols), BF)
    for place, block in enumerate(qkv_blocks):
        qkv_full = lax.dynamic_update_slice_in_dim(
            qkv_full, block[:, :cols], place * shard, axis=0
        )
    projected = nn(hidden, qkv_full)
    projected = projected.reshape(length, 3, heads, HD)
    normed_q, factor_q = normalize(projected[:, 0])
    normed_k, factor_k = normalize(projected[:, 1])
    queries = jnp.swapaxes(rotate(normed_q * gain_query, cosine, sine).astype(BF), 0, 1)
    keys = jnp.swapaxes(rotate(normed_k * gain_key, cosine, sine).astype(BF), 0, 1)
    values = jnp.swapaxes(projected[:, 2].astype(BF), 0, 1)
    scale = HD ** (-0.5)

    def bmm(left, right, dims):
        return lax.dot_general(left, right, (dims, ((0,), (0,))), preferred_element_type=F32)

    logits = jnp.where(same[None], bmm(queries, keys, ((2,), (2,))) * scale, NEG)
    powers = jnp.exp(logits - jnp.max(logits, axis=-1, keepdims=True))
    weights = powers / jnp.sum(powers, axis=-1, keepdims=True)
    weights_low = weights.astype(BF)
    attended = bmm(weights_low, values, ((2,), (1,))).astype(BF)
    merged = lax.all_to_all(
        jnp.swapaxes(attended, 0, 1), "seq", split_axis=0, concat_axis=1, tiled=True
    ).reshape(rows, H * HD)
    for e in range(min(local_experts, 3), local_experts):
        send_expert(e, attended)
    merged = to_relative(merged)

    inputs = tokens[0].astype(F32)
    residual = inputs + nn(merged[:, :half], out_even) + nn(merged[:, half:], out_odd)
    normed_f, factor_f = normalize(residual)
    hidden_own = (normed_f * gain_ffn).astype(BF)
    hidden_sent = by_chip(hidden_own)
    hidden_seq = lax.all_gather(hidden_sent, "seq", axis=0, tiled=True)
    forward_marks = [attended, merged, hidden_own]
    use_marks = [hidden_own, hidden_own]
    gate_ups = []
    downs = []
    for e in range(min(local_experts, 2)):
        gate_up, down = expert_weights(e, forward_marks[e], use_marks[e])
        gate_ups.append(gate_up)
        downs.append(down)
    hidden_two = jnp.concatenate([hidden_seq, swap(hidden_seq, 1)], axis=0)

    chances = jax.nn.softmax(nn(hidden_seq, router), axis=-1)
    picked = jnp.where(routed, chances, 0.0)
    picked_total = jnp.sum(picked, axis=1, keepdims=True)
    gates = picked / picked_total
    gates_seq = lax.dynamic_slice_in_dim(gates, seq_me * local_experts, local_experts, axis=1)
    gates_two = jnp.concatenate([gates_seq, swap(gates_seq, 1)], axis=0)

    grad_hidden_part = jnp.zeros((2 * length, model), F32)
    gate_grads = []
    wide_grads = []
    scaled_all = []
    for e in range(local_experts):
        gate = gates_two[:, e : e + 1]
        if e >= 2:
            mark = hidden_seq if e == 2 else wide_grads[e - 3]
            gate_up, down = expert_weights(e, mark, wide_grads[e - 2])
            gate_ups.append(gate_up)
            downs.append(down)
        before = nn(hidden_two, gate_ups[e])
        gate_part = before[:, : FF // 2]
        up_part = before[:, FF // 2 :]
        sigmoid_gate = jax.nn.sigmoid(gate_part)
        silu_gate = gate_part * sigmoid_gate
        activated = silu_gate * up_part
        scaled = (gate * activated).astype(BF)
        grad_act = nt(grad_two, downs[e])
        gate_grads.append(jnp.sum(grad_act * activated, axis=1, keepdims=True))
        grad_act = grad_act * gate
        grad_gate = grad_act * up_part * sigmoid_gate * (1.0 + gate_part * (1.0 - sigmoid_gate))
        grad_up = grad_act * silu_gate
        grad_before = jnp.concatenate([grad_gate, grad_up], axis=-1).astype(BF)
        grad_hidden_part = grad_hidden_part + nt(grad_before, gate_ups[e])
        wide_grads.append(grad_before)
        scaled_all.append(scaled)

    gate_grad_two = jnp.concatenate(gate_grads, axis=1)
    gate_grad_part = gate_grad_two[:length] + swap(gate_grad_two[length:], 1)
    gate_high, gate_low = split_two(gate_grad_part)
    grad_hidden_low = (
        grad_hidden_part[:length] + swap(grad_hidden_part[length:].astype(BF), 1).astype(F32)
    ).astype(BF)

    def spread(values):
        wide = jnp.zeros((length, experts), BF)
        return lax.dynamic_update_slice(wide, values, (0, seq_me * local_experts))

    payload = jnp.concatenate([grad_hidden_low, spread(gate_high), spread(gate_low)], axis=1)
    returned = lax.psum_scatter(payload, "seq", scatter_dimension=0, tiled=True)
    returned = returned.astype(F32)
    gate_grad = returned[:, model : model + experts] + returned[:, model + experts :]
    expert_parts = []

    def start_expert(e, anchor):
        wide = later(wide_grads[e], anchor)
        scaled = later(scaled_all[e], anchor)
        parts = [
            tn(hidden_two[:, mask * 2 * shard : (mask + 1) * 2 * shard], wide).astype(BF)
            for mask in range(chips)
        ]
        down_grad = tn(scaled, grad_two).astype(BF)
        down_parts = [
            lax.dynamic_slice_in_dim(down_grad, (chip ^ mask) * slim, slim, axis=0)
            for mask in range(chips)
        ]
        sent = send_first(parts, e % 2, chips)
        down_sent = send_first(down_parts, 1 - e % 2, chips)
        expert_parts.append((parts, sent, down_parts, down_sent))

    start_expert(0, payload)
    start_expert(1, payload)

    def finish_expert(e, anchor):
        parts, first, down_parts, down_first = expert_parts[e]
        summed = scatter_chips(parts, e % 2, chips, first, anchor).astype(BF)
        down_row = scatter_chips(down_parts, 1 - e % 2, chips, down_first, anchor)
        kept = lax.dynamic_slice_in_dim(summed, core * shard, shard, axis=0)
        sent = lax.dynamic_slice_in_dim(summed, (1 - core) * shard, shard, axis=0)
        got = swap(sent, 1)
        low_half = jnp.where(first_core, kept, got)
        high_half = jnp.where(first_core, got, kept)
        gate_up_row = jnp.concatenate(
            [
                source[:, j * slim : (j + 1) * slim]
                for j in range(wt_total)
                for source in (low_half, high_half)
            ],
            axis=1,
        ).astype(F32)
        return gate_up_row, down_row

    def own(full):
        return lax.dynamic_slice_in_dim(full, seq_me * rows, rows, axis=0)

    chances_own = own(chances)
    gates_own = own(gates)
    inner_gate = jnp.sum(gate_grad * gates_own, axis=1, keepdims=True)
    grad_chances = jnp.where(routed_own, (gate_grad - inner_gate) / own(picked_total), 0.0)
    grad_logits = (
        chances_own
        * (grad_chances - jnp.sum(grad_chances * chances_own, axis=1, keepdims=True))
    ).astype(BF)
    grad_hidden = by_chip(returned[:, :model] + nt(grad_logits, router))
    router_grad = tn(
        to_relative(hidden_own), jnp.pad(grad_logits, ((0, 0), (0, LANES - experts)))
    )
    ffn_gain_grad = jnp.sum(grad_hidden * normed_f, axis=0)
    grad_residual = cotangent[0].astype(F32) + norm_back(
        grad_hidden * gain_ffn, normed_f, factor_f
    )
    grad_branch = grad_residual.astype(BF)
    grad_merged = jnp.concatenate(
        [nt(grad_branch, out_even), nt(grad_branch, out_odd)], axis=1
    )
    grad_merged = from_relative(grad_merged.astype(BF))
    for e in range(2, min(local_experts, 3)):
        start_expert(e, grad_merged)
    grad_merged = grad_merged.reshape(rows, H, HD)
    grad_heads = jnp.swapaxes(
        lax.all_to_all(grad_merged, "seq", split_axis=1, concat_axis=0, tiled=True), 0, 1
    )

    scaled_out = [later(scaled, grad_heads) for scaled in scaled_all]
    out_part = jnp.zeros((2 * length, model), F32)
    for e in range(local_experts):
        out_part = out_part + nn(scaled_out[e], downs[e])
    out_other = swap(out_part[length:].astype(BF), 1)
    out_low = (out_part[:length] + out_other.astype(F32)).astype(BF)
    moe_out = lax.psum_scatter(out_low, "seq", scatter_dimension=0, tiled=True)
    moe_out = moe_out.astype(F32)

    def scatter_rows(left, right, route):
        sent = tn(left[:, half:], right).astype(BF)
        other = swap(sent, 1)
        kept = (tn(left[:, :half], right) + other.astype(F32)).astype(BF)
        parts = [kept[mask * shard : (mask + 1) * shard] for mask in range(chips)]
        first = send_first(parts, route, chips)
        return scatter_chips(parts, route, chips, first).astype(BF)

    out_sum = scatter_rows(later(merged, grad_merged), grad_branch, 1)

    out_grad = lax.psum(out_sum, "seq")
    out_grad = out_grad.astype(F32)

    grad_v = jnp.swapaxes(bmm(weights_low, grad_heads, ((1,), (1,))), 0, 1)
    grad_weights = bmm(grad_heads, values, ((2,), (2,)))
    inner = jnp.sum(weights * grad_weights, axis=-1, keepdims=True)
    grad_scores = (weights * (grad_weights - inner)).astype(BF)
    grad_q = jnp.swapaxes(bmm(grad_scores, keys, ((2,), (1,))), 0, 1) * scale
    grad_k = jnp.swapaxes(bmm(grad_scores, queries, ((1,), (1,))), 0, 1) * scale
    grad_q_normed = rotate(grad_q, cosine, -sine)
    grad_k_normed = rotate(grad_k, cosine, -sine)
    q_gain_grad = jnp.sum(grad_q_normed * normed_q, axis=(0, 1))
    k_gain_grad = jnp.sum(grad_k_normed * normed_k, axis=(0, 1))
    grad_q_raw = norm_back(grad_q_normed * gain_query, normed_q, factor_q)
    grad_k_raw = norm_back(grad_k_normed * gain_key, normed_k, factor_k)
    grads = [g.reshape(length, part).astype(BF) for g in (grad_q_raw, grad_k_raw, grad_v)]
    grad_projected = jnp.concatenate(grads, axis=1)
    grad_normed_part = nt(grad_projected, qkv_full)
    attn_gain_grad = jnp.sum(grad_normed_part * normed_all, axis=0)
    grad_normed_low = grad_normed_part.astype(BF)
    grad_normed_own = lax.psum_scatter(
        grad_normed_low, "seq", scatter_dimension=0, tiled=True
    )
    grad_normed_own = grad_normed_own.astype(F32)
    grad_normed_own = from_relative(grad_normed_own)
    normed_a, factor_a = normalize(inputs)
    tokens_grad = grad_residual + norm_back(grad_normed_own * gain_attn, normed_a, factor_a)

    def gain_line(vector):
        return jnp.pad(
            vector.reshape(wt_total, gain_part), ((0, 0), (0, shard - gain_part))
        ).reshape(model)

    lines = to_relative(
        jnp.stack([ffn_gain_grad, gain_line(q_gain_grad), gain_line(k_gain_grad)])
    )
    lines = jnp.concatenate([attn_gain_grad[None], lines, jnp.zeros((4, model), F32)], axis=0)
    small_grad = router_grad + tn(lines.astype(BF), jnp.asarray(picker, BF))
    small_sent = small_grad[half:].astype(BF)
    small_kept = (small_grad[:half] + swap(small_sent, 1).astype(F32)).astype(BF)
    small_sum = scatter_chips(
        [small_kept[mask * shard : (mask + 1) * shard] for mask in range(chips)], 1, chips
    ).astype(BF)
    for e in range(3, local_experts):
        start_expert(e, grad_normed_low)
    grads = [later(g, moe_out) for g in grads]
    value_sum = scatter_rows(hidden, grads[2], 0)
    query_sum = scatter_rows(hidden, grads[0], 1)
    key_sum = scatter_rows(hidden, grads[1], 0)
    collected_value = lax.all_gather(value_sum, "seq", axis=0)
    joined = jnp.concatenate([query_sum, key_sum, small_sum], axis=1)
    collected = lax.all_gather(joined, "seq", axis=0)
    qkv_out = jnp.concatenate(
        [collected[z, :, :part] for z in range(seq_total)]
        + [collected[z, :, part : 2 * part] for z in range(seq_total)]
        + [collected_value[z] for z in range(seq_total)],
        axis=1,
    ).astype(F32)
    small_out = jnp.sum(collected[:, :, 2 * part :].astype(F32), axis=0)
    anchors = [grad_heads, grad_projected, query_sum, key_sum]
    expert_rows = [
        finish_expert(e, anchors[min(e * len(anchors) // local_experts, len(anchors) - 1)])
        for e in range(local_experts)
    ]
    gate_up_out = jnp.stack([row[0] for row in expert_rows])
    down_out = jnp.stack([row[1] for row in expert_rows])
    output = (residual + moe_out + zero_of(grad_projected)).astype(BF)
    return (
        output[None],
        tokens_grad[None],
        qkv_out,
        out_grad,
        small_out[:, :experts],
        gate_up_out,
        down_out,
        small_out[:, experts],
        small_out[:, experts + 1],
        small_out[:gain_part, experts + 2],
        small_out[:gain_part, experts + 3],
    )


def solution(mesh):
    in_specs = (
        P("wt", "seq", None),
        P("wt", "seq", None),
        P("wt", None),
        P("wt", "seq", None),
        P("wt", None),
        P("wt", None),
        P("wt", None),
        P("seq", "wt", None),
        P("seq", "wt", None),
        P("wt"),
        P("wt"),
        P("wt"),
        P("wt"),
    )
    out_specs = (
        P("wt", "seq", None),
        P("wt", "seq", None),
        P("wt", None),
        P("wt", None),
        P("wt", None),
        P("seq", "wt", None),
        P("seq", "wt", None),
        P("wt"),
        P("wt"),
        P("wt"),
        P("wt"),
    )

    return jax.shard_map(body, mesh=mesh, in_specs=in_specs, out_specs=out_specs, check_vma=False)
```
